32 devices in a mesh: groups: 2 (over x), tm: 8 (over z, y), tile: 2 (over core).
Axes of the slice: x: 2, y: 2, z: 4, core: 2. Of those that a mesh axis runs over, the one named last changes fastest.
Arguments:
- movie: bfloat16 [4, 2304, 4096], P(('groups', 'tile'), None, 'tm'), parts along dimension 0, may hold values from 0 to 4
- cycle_weights: bfloat16 [4, 2304, 56], P(('groups', 'tile')), parts along dimension 0, may hold values from -0.75 to 0.75
- footprints: bfloat16 [4, 2304, 384], P(('groups', 'tile')), parts along dimension 0, may hold values from 0.19921875 to 1
- traces: bfloat16 [4, 384, 4096], P(('groups', 'tile'), None, 'tm'), parts along dimension 0, may hold values from 0 to 1.5
- centre_row: int32 [4, 384], P(('groups', 'tile')), parts along dimension 0, may hold values from 0 to 47
- centre_col: int32 [4, 384], P(('groups', 'tile')), parts along dimension 0, may hold values from 0 to 47
- radius: int32 [4, 384], P(('groups', 'tile')), parts along dimension 0, may hold values from 4 to 9
- comp_count: int32 [4], P(('groups', 'tile')), parts along dimension 0, may hold values from 64 to 384
Outputs:
- new_footprints: bfloat16 [4, 2304, 384], P(('groups', 'tile')), parts along dimension 0
- new_traces: bfloat16 [4, 384, 4096], P(('groups', 'tile'), None, 'tm'), parts along dimension 0
The draws below stay inside these ranges and needn't reach their ends.
There are 2 independent parts, one for each index of `groups`. The reference program is written for one: setup_inputs(seed, part) draws one part's arguments, and reference() takes and returns one part's arrays. A program takes and returns all parts, laid end to end along the dimension named above; each array names one. Nothing has to cross between parts.
All inputs are finite; a program needn't handle non-finite values.
Results may differ from the reference program's by a relative error of at most 0.0034.
Values may be sent and summed in bfloat16 or wider, within the bound.
A program may use at most 64 MiB of HBM per device.

```python
import math
import jax
import jax.numpy as jnp
from jax import lax

TILE_SIDE = 48
CYCLE = 8
OFFS = 56
KMAX = 384
PASSES = 2
PIX = 2304
TILES = 2
FRAMES = 4096


def draw_traces(key, part):
    first_key = jax.random.fold_in(jax.random.fold_in(key, 17), 0)
    ramp = 1.0 + 2.0 * jnp.arange(FRAMES, dtype=jnp.float32) / FRAMES
    logs = jax.random.uniform(first_key, (TILES, KMAX, FRAMES), jnp.float32, math.log(0.05), math.log(0.5))
    values = jnp.exp(logs) * ramp[None, None, :]
    return values.astype(jnp.bfloat16)


def place_ends(entries, stream_key, low, largest):
    dims = entries.shape
    index_at = [jax.random.randint(jax.random.fold_in(stream_key, axis), (), 0, dims[axis]) for axis in range(len(dims))]
    entries = entries.at[tuple(index_at)].set(low)
    longest = dims.index(max(dims))
    index_at[longest] = (index_at[longest] + 1) % dims[longest]
    return entries.at[tuple(index_at)].set(largest)


def steps_of(key, extent, shards, least, largest):
    gain, own = 1.0, jax.random.fold_in(key, 6)
    for position, blocks in shards:
        steps = jnp.exp(jax.random.uniform(jax.random.fold_in(own, position), (blocks,), jnp.float32, least / len(shards), largest / len(shards)))
        gain = gain * jnp.repeat(steps, extent[position] // blocks).reshape([-1 if axis == position else 1 for axis in range(len(extent))])
    return gain


def bell_draw(own_key, dims, spread, bound, pieces=(), held_as=jnp.bfloat16):
    array = jax.random.normal(own_key, dims, jnp.float32) * spread
    if len(pieces) > 0:
        array = steps_of(own_key, dims, pieces, -0.22, 0.18) * array
    return jnp.clip(array, min=-bound, max=bound).astype(held_as)


def setup_inputs(seed: int = 0, part: int = 0) -> dict:
    splits = jax.random.split(jax.random.key(seed), 9)
    own_keys = jax.random.split(jax.random.fold_in(splits[8], part), 9)
    return {
        "movie": jnp.clip(4.0 * jax.random.uniform(own_keys[0], (TILES, PIX, FRAMES), jnp.float32) ** steps_of(own_keys[0], (TILES, PIX, FRAMES), ((0, 2), (2, 8)), -0.2, 0.2), 0.0, 4.0).astype(jnp.bfloat16),
        "cycle_weights": bell_draw(own_keys[1], (TILES, PIX, OFFS), OFFS ** -0.5, 0.75, ((0, 2),)),
        "footprints": jnp.clip(0.19921875 + 0.80078125 * jax.random.uniform(own_keys[2], (TILES, PIX, KMAX), jnp.float32) ** steps_of(own_keys[2], (TILES, PIX, KMAX), ((0, 2),), -0.2, 0.2), 0.19921875, 1.0).astype(jnp.bfloat16),
        "traces": draw_traces(jax.random.fold_in(jax.random.fold_in(splits[8], part), 71), part),
        "centre_row": place_ends(jax.random.randint(own_keys[4], (TILES, KMAX), 0, TILE_SIDE), jax.random.fold_in(own_keys[4], 1), 0, TILE_SIDE - 1).astype(jnp.int32),
        "centre_col": place_ends(jax.random.randint(own_keys[5], (TILES, KMAX), 0, TILE_SIDE), jax.random.fold_in(own_keys[5], 1), 0, TILE_SIDE - 1).astype(jnp.int32),
        "radius": place_ends(jax.random.randint(own_keys[6], (TILES, KMAX), TILE_SIDE // 12, TILE_SIDE // 5 + 1), jax.random.fold_in(own_keys[6], 1), TILE_SIDE // 12, (TILE_SIDE // 5 + 1) - 1).astype(jnp.int32),
        "comp_count": jax.random.randint(own_keys[7], (TILES,), KMAX // 6, KMAX + 1).astype(jnp.int32),
    }


RIDGE_TERM = 1.0


def cycle_offsets():
    found = []
    for row_step in range(-CYCLE, CYCLE + 1):
        for col_step in range(-CYCLE, CYCLE + 1):
            dist_sq = row_step * row_step + col_step * col_step
            if CYCLE * CYCLE <= dist_sq < (CYCLE + 1) * (CYCLE + 1):
                found.append((row_step, col_step))
    return found


def cycle_back(weights, window):
    frames = window.shape[2]
    grid_w = weights.reshape(TILE_SIDE, TILE_SIDE, -1)
    total = jnp.zeros((TILE_SIDE, TILE_SIDE, frames), jnp.float32)
    for index, (row_step, col_step) in enumerate(cycle_offsets()):
        top = CYCLE + row_step
        left = CYCLE + col_step
        piece = window[top:top + TILE_SIDE, left:left + TILE_SIDE, :].astype(jnp.float32)
        total = total + grid_w[:, :, index:index + 1].astype(jnp.float32) * piece
    return total.reshape(TILE_SIDE * TILE_SIDE, frames).astype(jnp.bfloat16)


def keep_mask(row_at, col_at, reach, count):
    pixel = jnp.arange(TILE_SIDE * TILE_SIDE, dtype=jnp.int32)
    row_gap = (pixel // TILE_SIDE)[:, None] - row_at[None, :]
    col_gap = (pixel % TILE_SIDE)[:, None] - col_at[None, :]
    inside = row_gap * row_gap + col_gap * col_gap <= (reach * reach)[None, :]
    live = jnp.arange(KMAX, dtype=jnp.int32) < count
    return inside & live[None, :], live


def pad_tiles(resid):
    frames = resid.shape[2]
    blocks = resid.reshape(TILES, TILE_SIDE, TILE_SIDE, frames)
    field = jnp.transpose(blocks, (1, 0, 2, 3)).reshape(TILE_SIDE, TILES * TILE_SIDE, frames)
    padded = jnp.pad(field, ((CYCLE, CYCLE), (CYCLE, CYCLE), (0, 0)))
    pad_len = TILE_SIDE + 2 * CYCLE
    return [padded[:, tile_idx * TILE_SIDE:tile_idx * TILE_SIDE + pad_len, :] for tile_idx in range(TILES)]


def reference(movie, cycle_weights, footprints, traces, centre_row, centre_col, radius, comp_count):
    zero = jnp.zeros((), jnp.bfloat16)
    feet, lives, keeps, trace_now, den_a = [], [], [], [], []
    for tile_idx in range(TILES):
        keep, live = keep_mask(centre_row[tile_idx], centre_col[tile_idx], radius[tile_idx], comp_count[tile_idx])
        foot = jnp.where(keep, footprints[tile_idx], zero)
        feet.append(foot)
        keeps.append(keep)
        lives.append(live)
        trace_now.append(jnp.where(live[:, None], traces[tile_idx], zero))
        den_a.append(jnp.sum(jnp.square(foot.astype(jnp.float32)), axis=0) + RIDGE_TERM)
    movie_f = movie.astype(jnp.float32)
    backs = None
    for sweep in range(PASSES):
        prods = [jnp.dot(feet[tile_idx], trace_now[tile_idx], preferred_element_type=jnp.float32) for tile_idx in range(TILES)]
        resid = jnp.stack([(movie_f[tile_idx] - prods[tile_idx]).astype(jnp.bfloat16) for tile_idx in range(TILES)])
        windows = pad_tiles(resid)
        backs = [cycle_back(cycle_weights[tile_idx], windows[tile_idx]) for tile_idx in range(TILES)]
        updated = []
        for tile_idx in range(TILES):
            err = (prods[tile_idx] + backs[tile_idx].astype(jnp.float32) - movie_f[tile_idx]).astype(jnp.bfloat16)
            grad = lax.dot_general(feet[tile_idx], err, (((0,), (0,)), ((), ())), preferred_element_type=jnp.float32)
            moved = jnp.maximum(trace_now[tile_idx].astype(jnp.float32) - grad / den_a[tile_idx][:, None], 0.0)
            updated.append(jnp.where(lives[tile_idx][:, None], moved, 0.0).astype(jnp.bfloat16))
        trace_now = updated
    outs_a = []
    for tile_idx in range(TILES):
        prod = jnp.dot(feet[tile_idx], trace_now[tile_idx], preferred_element_type=jnp.float32)
        ferr = (prod + backs[tile_idx].astype(jnp.float32) - movie_f[tile_idx]).astype(jnp.bfloat16)
        grad_a = lax.dot_general(ferr, trace_now[tile_idx], (((1,), (1,)), ((), ())), preferred_element_type=jnp.float32)
        den_c = jnp.sum(jnp.square(trace_now[tile_idx].astype(jnp.float32)), axis=1) + RIDGE_TERM
        moved = jnp.maximum(feet[tile_idx].astype(jnp.float32) - grad_a / den_c[None, :], 0.0)
        outs_a.append(jnp.where(keeps[tile_idx], moved, 0.0).astype(jnp.bfloat16))
    return jnp.stack(outs_a), jnp.stack(trace_now)
```

```python
import functools

import jax
import jax.numpy as jnp
import numpy as np
from jax import lax
from jax.experimental import pallas as pl
from jax.experimental.pallas import tpu as pltpu
from jax.sharding import PartitionSpec as P

SIDE = 48
CYCLE = 8
PASSES = 2
RIDGE_TERM = 1.0
EDGE = 16
TILES = SIDE // EDGE
SPAN = EDGE + 2 * CYCLE
LANES = 128
STEP = LANES // SPAN
CHUNKS = (STEP - 1 + 2 * CYCLE) // STEP + 1
FOLD_ROWS = 24
SHIFT = FOLD_ROWS // 2
F32 = jnp.float32
BF16 = jnp.bfloat16
MESH = pl.DeviceIdType.MESH


def cycle_offsets():
    found = []
    for row_step in range(-CYCLE, CYCLE + 1):
        for col_step in range(-CYCLE, CYCLE + 1):
            dist_sq = row_step * row_step + col_step * col_step
            if CYCLE * CYCLE <= dist_sq < (CYCLE + 1) * (CYCLE + 1):
                found.append((row_step, col_step))
    return found


def tap_tables():
    offsets = {step: index for index, step in enumerate(cycle_offsets())}
    tables = np.full((STEP, CHUNKS, EDGE, LANES), len(offsets), np.int32)
    for phase in range(STEP):
        for chunk in range(CHUNKS):
            for col in range(EDGE):
                for lane in range(LANES):
                    row_step = chunk * STEP + lane // SPAN - phase - CYCLE
                    col_step = lane % SPAN - col - CYCLE
                    if (row_step, col_step) in offsets:
                        tables[phase, chunk, col, lane] = offsets[(row_step, col_step)]
    return tables


def kernel(
    n, s, shares,
    movie_in, stored_in, prints_in, traces_in, row_in, col_in, reach_in, count, tables_in,
    packed, new_trace,
    movie, stored, prints, trace, row_at, col_at, reach, tables,
    weights, foot, band, pm, win, errs, backs, inv_den,
    halo_out, halo_in, part, own, arrived, energy_out, energy_in, gathered,
    load_sems, small_sems, halo_sems, part_sems, energy_sems, gather_sems, out_sems,
):
    me = lax.axis_index("tm")
    tile = lax.axis_index("tile")
    frames = movie.shape[3]
    comps = foot.shape[3]
    pixels = SIDE * SIDE

    def load(b, j, kind):
        source, target = ((prints_in, prints), (movie_in, movie))[kind]
        rows = slice(b * EDGE, (b + 1) * EDGE)
        return pltpu.make_async_copy(
            source.at[rows, j * EDGE : (j + 1) * EDGE], target.at[j, rows], load_sems.at[kind, b, j]
        )

    smalls = [
        pltpu.make_async_copy(source, target, small_sems.at[index])
        for index, (source, target) in enumerate((
            (row_in, row_at), (col_in, col_at), (reach_in, reach),
            (stored_in, stored), (tables_in, tables), (traces_in, trace),
        ))
    ]
    for copy in smalls:
        copy.start()
    for b in range(TILES):
        for kind in range(2):
            for j in range(TILES):
                load(b, j, kind).start()

    barrier = pltpu.get_barrier_semaphore()
    pl.semaphore_signal(barrier, inc=1, device_id={"tile": 1 - tile}, device_id_type=MESH)

    def greet(t, carry):
        peer = lax.rem(me + 1 + t, n)
        pl.semaphore_signal(barrier, inc=1, device_id={"tm": peer}, device_id_type=MESH)
        return carry

    lax.fori_loop(0, n - 1, greet, 0)

    blank = jnp.zeros((SIDE, CYCLE, frames), BF16)
    for sweep in range(PASSES):
        win[sweep, :, 0, 0:CYCLE] = blank
        win[sweep, :, TILES, CYCLE:EDGE] = blank

    for copy in smalls:
        copy.wait()
    live_row = lax.broadcasted_iota(jnp.int32, (1, comps), 1) < count[0]
    bound = jnp.where(live_row, reach[...] * reach[...], -1)
    live = lax.broadcasted_iota(jnp.int32, (comps, LANES), 0) < count[0]
    for q in range(frames // LANES):
        cols = slice(q * LANES, (q + 1) * LANES)
        trace[:, cols] = jnp.where(live, trace[:, cols].astype(F32), 0.0).astype(BF16)

    taps = stored.shape[0]
    run = CYCLE * SIDE
    for b in range(SIDE // CYCLE):
        values = stored[:, b * run : (b + 1) * run].astype(F32)
        values = jnp.concatenate([values, jnp.zeros((LANES - taps, run), F32)], axis=0)
        weights[b * CYCLE : (b + 1) * CYCLE] = jnp.transpose(values).reshape(CYCLE, TILES, EDGE, LANES)

    col_sq = []
    for j in range(TILES):
        gap = lax.broadcasted_iota(jnp.int32, (EDGE, comps), 0) + j * EDGE - col_at[...]
        col_sq.append(gap * gap)

    def store_window(sweep, rows, j, diff):
        resid = (-diff).astype(BF16)
        win[sweep, rows, j, CYCLE:EDGE] = resid[:, 0:CYCLE]
        win[sweep, rows, j + 1, 0:CYCLE] = resid[:, CYCLE:EDGE]

    def opening(b):
        def step(q, total):
            for phase in range(STEP):
                r = b * EDGE + q * STEP + phase
                spot = pl.multiple_of((q * STEP + phase) * EDGE, EDGE)
                row_gap = r - row_at[...]
                edge = bound - row_gap * row_gap
                for j in range(TILES):
                    kept = jnp.where(col_sq[j] <= edge, prints[j, r].astype(F32), 0.0)
                    foot[j, r] = kept.astype(BF16)
                    total = total + kept * kept
                    held = weights[r, j]
                    for chunk in range(CHUNKS):
                        found = [
                            jnp.take_along_axis(
                                held[h * 8 : h * 8 + 8], tables[phase, chunk, h * 8 : h * 8 + 8], axis=1
                            )
                            for h in range(EDGE // 8)
                        ]
                        lane = pl.multiple_of((q + chunk) * LANES, LANES)
                        band[j, b, pl.ds(spot, EDGE), pl.ds(lane, LANES)] = jnp.concatenate(found, axis=0).astype(BF16)
                    for chunk in range(CHUNKS, SPAN // STEP):
                        lane = pl.multiple_of(lax.rem(q + chunk, SPAN // STEP) * LANES, LANES)
                        band[j, b, pl.ds(spot, EDGE), pl.ds(lane, LANES)] = jnp.zeros((EDGE, LANES), BF16)
            rows = pl.ds(b * EDGE + q * STEP, STEP)
            feet = foot[:, rows].reshape(TILES * STEP * EDGE, comps)
            prod = jnp.dot(feet, trace[...], preferred_element_type=F32)
            prod = prod.reshape(TILES, STEP, EDGE, frames)
            for j in range(TILES):
                diff = prod[j] - movie[j, rows].astype(F32)
                pm[j, rows] = diff
                store_window(0, rows, j, diff)
            return total

        return step

    total = jnp.zeros((EDGE, comps), F32)
    for b in range(TILES):
        for kind in range(2):
            for j in range(TILES):
                load(b, j, kind).wait()
        total = lax.fori_loop(0, EDGE // STEP, opening(b), total)
    den = jnp.sum(total, axis=0, keepdims=True) + RIDGE_TERM
    inv_den[...] = jnp.transpose(jnp.broadcast_to(1.0 / den, (LANES, comps)))

    def halo_copy(sweep):
        return pltpu.make_async_remote_copy(
            src_ref=halo_out.at[sweep],
            dst_ref=halo_in.at[sweep],
            send_sem=halo_sems.at[0, sweep],
            recv_sem=halo_sems.at[1, sweep],
            device_id={"tile": 1 - tile},
            device_id_type=MESH,
        )

    def send_halo(sweep, diff):
        cut = jnp.where(tile == 0, diff[:, CYCLE:EDGE], diff[:, 0:CYCLE])
        halo_out[sweep] = (-cut).reshape(SIDE * CYCLE, frames).astype(BF16)
        halo_copy(sweep).start()

    near = [jnp.where(tile == 0, TILES - 1 - t, t) for t in range(TILES)]
    for sweep in range(PASSES):
        if sweep == 0:
            pl.semaphore_wait(barrier, n)
            send_halo(0, pm[near[0]])
        else:
            for t in range(TILES):
                j = near[t]
                prod = jnp.dot(
                    foot[j].reshape(SIDE * EDGE, comps), trace[...], preferred_element_type=F32
                )
                diff = prod.reshape(SIDE, EDGE, frames) - movie[j].astype(F32)
                pm[j] = diff
                store_window(sweep, slice(0, SIDE), j, diff)
                if t == 0:
                    send_halo(sweep, diff)

        for t in range(TILES):
            j = near[TILES - 1 - t]
            if t == TILES - 1:
                halo_copy(sweep).wait_recv()
                came = halo_in[sweep].astype(F32).reshape(SIDE, CYCLE, frames).astype(BF16)

                @pl.when(tile == 0)
                def _():
                    win[sweep, :, TILES, CYCLE:EDGE] = came

                @pl.when(tile != 0)
                def _():
                    win[sweep, :, 0, 0:CYCLE] = came

            for b in range(TILES):
                first = b * EDGE - CYCLE
                low, high = max(first, 0), min(first + SPAN, SIDE)
                seen = win[sweep, low:high, pl.ds(j, 2)].reshape((high - low) * SPAN, frames)
                taken = band[j, b, :, (low - first) * SPAN : (high - first) * SPAN]
                back = jnp.dot(taken, seen, preferred_element_type=F32).astype(BF16)
                back = back.reshape(EDGE, EDGE, frames)
                rows = slice(b * EDGE, (b + 1) * EDGE)
                if sweep == PASSES - 1:
                    backs[j, rows] = back
                errs[j, rows] = (pm[j, rows] + back.astype(F32)).astype(BF16)

        grad = lax.dot_general(
            foot[...].reshape(pixels, comps),
            errs[...].reshape(pixels, frames),
            (((0,), (0,)), ((), ())),
            preferred_element_type=F32,
        )
        for q in range(frames // LANES):
            cols = slice(q * LANES, (q + 1) * LANES)
            moved = jnp.maximum(trace[:, cols].astype(F32) - grad[:, cols] * inv_den[...], 0.0)
            trace[:, cols] = jnp.where(live, moved, 0.0).astype(BF16)

    trace_copy = pltpu.make_async_copy(trace, new_trace, out_sems.at[0])
    trace_copy.start()
    squares = jnp.zeros((comps, LANES), F32)
    for q in range(frames // LANES):
        now = trace[:, q * LANES : (q + 1) * LANES].astype(F32)
        squares = squares + now * now
    energy = jnp.sum(jnp.transpose(squares), axis=0, keepdims=True)
    energy_out[...] = jnp.broadcast_to(energy, energy_out.shape)

    def energy_copy(peer, sender):
        return pltpu.make_async_remote_copy(
            src_ref=energy_out,
            dst_ref=energy_in.at[sender],
            send_sem=energy_sems.at[0, peer],
            recv_sem=energy_sems.at[1, sender],
            device_id={"tm": peer},
            device_id_type=MESH,
        )

    def part_copy(peer, sender):
        return pltpu.make_async_remote_copy(
            src_ref=part.at[peer],
            dst_ref=arrived.at[sender],
            send_sem=part_sems.at[0, peer],
            recv_sem=part_sems.at[1, sender],
            device_id={"tm": peer},
            device_id_type=MESH,
        )

    def gather_copy(peer, sender):
        return pltpu.make_async_remote_copy(
            src_ref=gathered.at[sender],
            dst_ref=gathered.at[sender],
            send_sem=gather_sems.at[0, peer],
            recv_sem=gather_sems.at[1, sender],
            device_id={"tm": peer},
            device_id_type=MESH,
        )

    def owns(index, do):
        if shares == n:
            do()
        else:
            pl.when(index < shares)(do)

    def over_peers(do):
        def step(t, carry):
            do(lax.rem(me + 1 + t, n))
            return carry

        lax.fori_loop(0, n - 1, step, 0)

    over_peers(lambda peer: owns(peer, lambda: energy_copy(peer, me).start()))

    def rows_of(ref, share):
        found = []
        for j in range(TILES):
            first = share * s if j % 2 == 0 else lax.rem(share * s + SHIFT, FOLD_ROWS)
            for lap in range(SIDE // FOLD_ROWS):
                found.append(ref[j, pl.ds(first + lap * FOLD_ROWS, s)])
        found = jnp.concatenate(found, axis=0)
        return found.reshape(found.shape[0] * EDGE, ref.shape[3])

    def fold(values):
        return jnp.sum(values.reshape(-1, s * EDGE, comps), axis=0)

    def share_of(share):
        feet = rows_of(foot, share)
        prod = jnp.dot(feet, trace[...], preferred_element_type=F32)
        ferr = prod + rows_of(backs, share).astype(F32) - rows_of(movie, share).astype(F32)
        grad = lax.dot_general(
            ferr.astype(BF16), trace[...], (((1,), (1,)), ((), ())), preferred_element_type=F32
        )
        return fold(jnp.where(feet.astype(F32) > 0.0, grad, 0.0))

    def send_share(share):
        part[share] = share_of(share).astype(BF16)
        part_copy(share, me).start()

    over_peers(lambda peer: owns(peer, lambda: send_share(peer)))

    def settle():
        own[...] = share_of(me)
        energy_in[me] = energy_out[...]

        def take(peer):
            energy_copy(me, peer).wait_recv()
            part_copy(me, peer).wait_recv()
            own[...] += arrived[peer].astype(F32)
            energy_in[me] += energy_in[peer]

        over_peers(take)
        den_c = energy_in[me][:1] + RIDGE_TERM
        feet = fold(rows_of(foot, me).astype(F32))
        gathered[me] = jnp.maximum(feet - own[...] / den_c, 0.0).astype(BF16)
        over_peers(lambda peer: gather_copy(peer, me).start())

    owns(me, settle)
    over_peers(lambda peer: owns(peer, lambda: gather_copy(me, peer).wait_recv()))
    packed_copy = pltpu.make_async_copy(gathered.at[0:shares], packed, out_sems.at[1])
    packed_copy.start()

    for sweep in range(PASSES):
        halo_copy(sweep).wait_send()

    def drain(peer):
        owns(peer, lambda: energy_copy(peer, me).wait_send())
        owns(peer, lambda: part_copy(peer, me).wait_send())
        owns(me, lambda: gather_copy(peer, me).wait_send())

    over_peers(drain)
    trace_copy.wait()
    packed_copy.wait()


def unfold(
    s, packed_in, trace_in, row_in, col_in, reach_in, count,
    new_foot, new_trace,
    packed, trace, row_at, col_at, reach, values, feet, load_sems, foot_sems,
):
    comps = feet.shape[2]
    loads = [
        pltpu.make_async_copy(source, target, load_sems.at[index])
        for index, (source, target) in enumerate((
            (packed_in, packed), (trace_in, trace), (row_in, row_at), (col_in, col_at), (reach_in, reach),
        ))
    ]
    for copy in loads:
        copy.start()
    for index in (0, 2, 3, 4):
        loads[index].wait()
    live = lax.broadcasted_iota(jnp.int32, (1, comps), 1) < count[0]
    bound = jnp.where(live, reach[...] * reach[...], -1)
    for r in range(FOLD_ROWS):
        values[r] = packed[r // s, r % s * EDGE : (r % s + 1) * EDGE].astype(F32)
    loads[1].wait()
    trace_copy = pltpu.make_async_copy(trace, new_trace, load_sems.at[1])
    trace_copy.start()
    col_sq = []
    for j in range(TILES):
        gap = lax.broadcasted_iota(jnp.int32, (EDGE, comps), 0) + j * EDGE - col_at[...]
        col_sq.append(gap * gap)

    def row(r):
        row_gap = r - row_at[...]
        edge = bound - row_gap * row_gap
        for j in range(TILES):
            value = values[lax.rem(r + j % 2 * SHIFT, FOLD_ROWS)]
            feet[r, j * EDGE : (j + 1) * EDGE] = jnp.where(col_sq[j] <= edge, value, 0.0).astype(BF16)

    copies = []
    for b in range(TILES):
        def step(t, carry):
            for u in range(2):
                row(b * EDGE + t * 2 + u)
            return carry

        lax.fori_loop(0, EDGE // 2, step, 0)
        rows = slice(b * EDGE, (b + 1) * EDGE)
        copies.append(pltpu.make_async_copy(feet.at[rows], new_foot.at[rows], foot_sems.at[b]))
        copies[-1].start()
    for copy in copies:
        copy.wait()
    trace_copy.wait()


def shards(movie, cycle_weights, footprints, traces, centre_row, centre_col, radius, comp_count):
    n = lax.axis_size("tm")
    frames = movie.shape[2]
    comps = footprints.shape[2]
    taps = cycle_weights.shape[2]
    s = -(-FOLD_ROWS // n)
    while SHIFT % s:
        s += 1
    shares = FOLD_ROWS // s
    anyspace = pl.BlockSpec(memory_space=pl.ANY)
    smem = pl.BlockSpec(memory_space=pltpu.SMEM)
    dma = pltpu.SemaphoreType.DMA
    packed, trace = pl.pallas_call(
        functools.partial(kernel, n, s, shares),
        out_shape=(
            jax.ShapeDtypeStruct((shares, s * EDGE, comps), BF16),
            jax.ShapeDtypeStruct((comps, frames), BF16),
        ),
        in_specs=[anyspace] * 7 + [smem, anyspace],
        out_specs=(anyspace, anyspace),
        scratch_shapes=[
            pltpu.VMEM((TILES, SIDE, EDGE, frames), BF16),
            pltpu.VMEM((taps, SIDE * SIDE), BF16),
            pltpu.VMEM((TILES, SIDE, EDGE, comps), BF16),
            pltpu.VMEM((comps, frames), BF16),
            pltpu.VMEM((1, comps), jnp.int32),
            pltpu.VMEM((1, comps), jnp.int32),
            pltpu.VMEM((1, comps), jnp.int32),
            pltpu.VMEM((STEP, CHUNKS, EDGE, LANES), jnp.int32),
            pltpu.VMEM((SIDE, TILES, EDGE, LANES), F32),
            pltpu.VMEM((TILES, SIDE, EDGE, comps), BF16),
            pltpu.VMEM((TILES, TILES, EDGE * EDGE, SPAN * SPAN), BF16),
            pltpu.VMEM((TILES, SIDE, EDGE, frames), F32),
            pltpu.VMEM((PASSES, SIDE, TILES + 1, EDGE, frames), BF16),
            pltpu.VMEM((TILES, SIDE, EDGE, frames), BF16),
            pltpu.VMEM((TILES, SIDE, EDGE, frames), BF16),
            pltpu.VMEM((comps, LANES), F32),
            pltpu.VMEM((PASSES, SIDE * CYCLE, frames), BF16),
            pltpu.VMEM((PASSES, SIDE * CYCLE, frames), BF16),
            pltpu.VMEM((n, s * EDGE, comps), BF16),
            pltpu.VMEM((s * EDGE, comps), F32),
            pltpu.VMEM((n, s * EDGE, comps), BF16),
            pltpu.VMEM((8, comps), F32),
            pltpu.VMEM((n, 8, comps), F32),
            pltpu.VMEM((n, s * EDGE, comps), BF16),
            dma((2, TILES, TILES)),
            dma((6,)),
            dma((2, PASSES)),
            dma((2, n)),
            dma((2, n)),
            dma((2, n)),
            dma((2,)),
        ],
        compiler_params=pltpu.CompilerParams(
            collective_id=0, has_side_effects=True, vmem_limit_bytes=60 * 1024 * 1024
        ),
    )(
        movie.reshape(SIDE, SIDE, frames),
        jnp.transpose(cycle_weights[0]),
        footprints.reshape(SIDE, SIDE, comps),
        traces.reshape(comps, frames),
        centre_row,
        centre_col,
        radius,
        comp_count,
        jnp.asarray(tap_tables()),
    )
    new_foot, new_trace = pl.pallas_call(
        functools.partial(unfold, s),
        out_shape=(
            jax.ShapeDtypeStruct((SIDE, SIDE, comps), BF16),
            jax.ShapeDtypeStruct((comps, frames), BF16),
        ),
        in_specs=[anyspace] * 5 + [smem],
        out_specs=(anyspace, anyspace),
        scratch_shapes=[
            pltpu.VMEM((shares, s * EDGE, comps), BF16),
            pltpu.VMEM((comps, frames), BF16),
            pltpu.VMEM((1, comps), jnp.int32),
            pltpu.VMEM((1, comps), jnp.int32),
            pltpu.VMEM((1, comps), jnp.int32),
            pltpu.VMEM((FOLD_ROWS, EDGE, comps), F32),
            pltpu.VMEM((SIDE, SIDE, comps), BF16),
            dma((5,)),
            dma((TILES,)),
        ],
    )(packed, trace, centre_row, centre_col, radius, comp_count)
    return (new_foot.reshape(1, SIDE * SIDE, comps), new_trace[None])


def solution(mesh):
    in_specs = (
        P(("groups", "tile"), None, "tm"),
        P(("groups", "tile"), None, None),
        P(("groups", "tile"), None, None),
        P(("groups", "tile"), None, "tm"),
        P(("groups", "tile"), None),
        P(("groups", "tile"), None),
        P(("groups", "tile"), None),
        P(("groups", "tile")),
    )
    out_specs = (P(("groups", "tile"), None, None), P(("groups", "tile"), None, "tm"))
    return jax.shard_map(shards, mesh=mesh, in_specs=in_specs, out_specs=out_specs, check_vma=False)
```

```python
import functools

import jax
import jax.numpy as jnp
import numpy as np
from jax import lax
from jax.experimental import pallas as pl
from jax.experimental.pallas import tpu as pltpu
from jax.sharding import PartitionSpec as P

SIDE = 48
CYCLE = 8
PASSES = 2
RIDGE_TERM = 1.0
EDGE = 16
TILES = SIDE // EDGE
SPAN = EDGE + 2 * CYCLE
LANES = 128
STEP = LANES // SPAN
CHUNKS = (STEP - 1 + 2 * CYCLE) // STEP + 1
FOLD_ROWS = 19
SHIFT = 9
TEAM_ROWS = 4
ORDER = -1
F32 = jnp.float32
BF16 = jnp.bfloat16
MESH = pl.DeviceIdType.MESH


def cycle_offsets():
    found = []
    for row_step in range(-CYCLE, CYCLE + 1):
        for col_step in range(-CYCLE, CYCLE + 1):
            dist_sq = row_step * row_step + col_step * col_step
            if CYCLE * CYCLE <= dist_sq < (CYCLE + 1) * (CYCLE + 1):
                found.append((row_step, col_step))
    return found


def tap_tables():
    offsets = {step: index for index, step in enumerate(cycle_offsets())}
    tables = np.full((STEP, CHUNKS, EDGE, LANES), len(offsets), np.int16)
    for phase in range(STEP):
        for chunk in range(CHUNKS):
            for col in range(EDGE):
                for lane in range(LANES):
                    row_step = chunk * STEP + lane // SPAN - phase - CYCLE
                    col_step = lane % SPAN - col - CYCLE
                    if (row_step, col_step) in offsets:
                        tables[phase, chunk, col, lane] = offsets[(row_step, col_step)]
    return tables


def share_bounds(n):
    base, extra = divmod(FOLD_ROWS, n)
    bounds = [0]
    for index in range(n):
        bounds.append(bounds[-1] + base + (index >= n - extra))
    return bounds


def share_teams(bounds):
    teams, held = [], []
    for share in range(len(bounds) - 1):
        if bounds[share] < bounds[share + 1]:
            held.append(share)
        if held and bounds[share + 1] - bounds[held[0]] >= TEAM_ROWS:
            teams.append(held)
            held = []
    return teams + [held] if held else teams


def fold_runs(first, last):
    runs = []
    for j in range(TILES):
        for lap in range(-TILES, TILES + 1):
            moved = SHIFT * j + FOLD_ROWS * lap
            low, high = max(first + moved, 0), min(last + moved, SIDE)
            if low < high:
                runs.append((j, low, high, low - moved))
    return runs


def pick(values, index):
    numbers = lax.GatherDimensionNumbers(
        offset_dims=(), collapsed_slice_dims=(1,), start_index_map=(1,),
        operand_batching_dims=(0,), start_indices_batching_dims=(0,),
    )
    inside = lax.GatherScatterMode.PROMISE_IN_BOUNDS
    return lax.gather(values, index[..., None], numbers, (1, 1), mode=inside)


def kernel(
    n, bounds,
    movie_in, stored_in, prints_in, traces_in, row_in, col_in, reach_in, count, tables_in,
    packed, new_trace,
    movie, stored, prints, trace, row_at, col_at, reach, tables,
    weights, foot, band, pm, win, errs, backs, inv_den,
    halo_out, halo_in, part, own, arrived, energy_out, energy_in, gathered,
    load_sems, small_sems, halo_sems, part_sems, energy_sems, gather_sems, out_sems,
):
    me = lax.axis_index("tm")
    tile = lax.axis_index("tile")
    frames = movie.shape[3]
    comps = foot.shape[3]
    pixels = SIDE * SIDE

    def load(b, j, kind):
        source, target = ((prints_in, prints), (movie_in, movie))[kind]
        rows = slice(b * EDGE, (b + 1) * EDGE)
        return pltpu.make_async_copy(
            source.at[rows, j * EDGE : (j + 1) * EDGE], target.at[j, rows], load_sems.at[kind, b, j]
        )

    smalls = [
        pltpu.make_async_copy(source, target, small_sems.at[index])
        for index, (source, target) in enumerate((
            (row_in, row_at), (col_in, col_at), (reach_in, reach),
            (stored_in, stored), (tables_in, tables), (traces_in, trace),
        ))
    ]
    for copy in smalls:
        copy.start()
    for b in range(TILES):
        for kind in range(2):
            for j in range(TILES):
                load(b, j, kind).start()

    barrier = pltpu.get_barrier_semaphore()
    pl.semaphore_signal(barrier, inc=1, device_id={"tile": 1 - tile}, device_id_type=MESH)

    def greet(t, carry):
        peer = lax.rem(me + 1 + t, n)
        pl.semaphore_signal(barrier, inc=1, device_id={"tm": peer}, device_id_type=MESH)
        return carry

    lax.fori_loop(0, n - 1, greet, 0)

    blank = jnp.zeros((SIDE, CYCLE, frames), BF16)
    for sweep in range(PASSES):
        win[sweep, :, 0, 0:CYCLE] = blank
        win[sweep, :, TILES, CYCLE:EDGE] = blank

    for copy in smalls:
        copy.wait()
    live_row = lax.broadcasted_iota(jnp.int32, (1, comps), 1) < count[0]
    bound = jnp.where(live_row, reach[...] * reach[...], -1)
    live = lax.broadcasted_iota(jnp.int32, (comps, LANES), 0) < count[0]
    for q in range(frames // LANES):
        cols = slice(q * LANES, (q + 1) * LANES)
        trace[:, cols] = jnp.where(live, trace[:, cols].astype(F32), 0.0).astype(BF16)

    col_sq = []
    for j in range(TILES):
        gap = lax.broadcasted_iota(jnp.int32, (EDGE, comps), 0) + j * EDGE - col_at[...]
        col_sq.append(gap * gap)

    def store_window(sweep, rows, j, diff):
        resid = (-diff).astype(BF16)
        win[sweep, rows, j, CYCLE:EDGE] = resid[:, 0:CYCLE]
        win[sweep, rows, j + 1, 0:CYCLE] = resid[:, CYCLE:EDGE]

    def opening(b):
        def step(q, total):
            for phase in range(STEP):
                r = b * EDGE + q * STEP + phase
                spot = pl.multiple_of((q * STEP + phase) * EDGE, EDGE)
                row_gap = r - row_at[...]
                edge = bound - row_gap * row_gap
                for j in range(TILES):
                    kept = jnp.where(col_sq[j] <= edge, prints[j, r].astype(F32), 0.0)
                    foot[j, r] = kept.astype(BF16)
                    total = total + kept * kept
                    held = weights[r, j]
                    for chunk in range(CHUNKS):
                        lane = pl.multiple_of((q + chunk) * LANES, LANES)
                        band[j, b, pl.ds(spot, EDGE), pl.ds(lane, LANES)] = pick(held, tables[phase, chunk])
                    for chunk in range(CHUNKS, SPAN // STEP):
                        lane = pl.multiple_of(lax.rem(q + chunk, SPAN // STEP) * LANES, LANES)
                        band[j, b, pl.ds(spot, EDGE), pl.ds(lane, LANES)] = jnp.zeros((EDGE, LANES), BF16)
            rows = pl.ds(b * EDGE + q * STEP, STEP)
            feet = foot[:, rows].reshape(TILES * STEP * EDGE, comps)
            prod = jnp.dot(feet, trace[...], preferred_element_type=F32)
            prod = prod.reshape(TILES, STEP, EDGE, frames)
            for j in range(TILES):
                diff = prod[j] - movie[j, rows].astype(F32)
                pm[j, rows] = diff
                store_window(0, rows, j, diff)
            return total

        return step

    taps = stored.shape[0]
    run = CYCLE * SIDE
    total = jnp.zeros((EDGE, comps), F32)
    for b in range(TILES):
        for h in range(b * EDGE // CYCLE, (b + 1) * EDGE // CYCLE):
            values = stored[:, h * run : (h + 1) * run].astype(F32)
            values = jnp.concatenate([values, jnp.zeros((LANES - taps, run), F32)], axis=0)
            turned = jnp.transpose(values).astype(BF16)
            weights[h * CYCLE : (h + 1) * CYCLE] = turned.reshape(CYCLE, TILES, EDGE, LANES)
        for kind in range(2):
            for j in range(TILES):
                load(b, j, kind).wait()
        total = lax.fori_loop(0, EDGE // STEP, opening(b), total)
    den = jnp.sum(total, axis=0, keepdims=True) + RIDGE_TERM
    inv_den[...] = jnp.transpose(jnp.broadcast_to(1.0 / den, (LANES, comps)))

    def halo_copy(sweep):
        return pltpu.make_async_remote_copy(
            src_ref=halo_out.at[sweep],
            dst_ref=halo_in.at[sweep],
            send_sem=halo_sems.at[0, sweep],
            recv_sem=halo_sems.at[1, sweep],
            device_id={"tile": 1 - tile},
            device_id_type=MESH,
        )

    def send_halo(sweep, diff):
        cut = jnp.where(tile == 0, diff[:, CYCLE:EDGE], diff[:, 0:CYCLE])
        halo_out[sweep] = (-cut).reshape(SIDE * CYCLE, frames).astype(BF16)
        halo_copy(sweep).start()

    near = [jnp.where(tile == 0, TILES - 1 - t, t) for t in range(TILES)]
    for sweep in range(PASSES):
        if sweep == 0:
            pl.semaphore_wait(barrier, n)
            send_halo(0, pm[near[0]])
        else:
            for t in range(TILES):
                j = near[t]
                prod = jnp.dot(
                    foot[j].reshape(SIDE * EDGE, comps), trace[...], preferred_element_type=F32
                )
                diff = prod.reshape(SIDE, EDGE, frames) - movie[j].astype(F32)
                pm[j] = diff
                store_window(sweep, slice(0, SIDE), j, diff)
                if t == 0:
                    send_halo(sweep, diff)

        for t in range(TILES):
            j = near[TILES - 1 - t]
            if t == TILES - 1:
                halo_copy(sweep).wait_recv()
                came = halo_in[sweep].astype(F32).reshape(SIDE, CYCLE, frames).astype(BF16)

                @pl.when(tile == 0)
                def _():
                    win[sweep, :, TILES, CYCLE:EDGE] = came

                @pl.when(tile != 0)
                def _():
                    win[sweep, :, 0, 0:CYCLE] = came

            for b in range(TILES):
                first = b * EDGE - CYCLE
                low, high = max(first, 0), min(first + SPAN, SIDE)
                seen = win[sweep, low:high, pl.ds(j, 2)].reshape((high - low) * SPAN, frames)
                taken = band[j, b, :, (low - first) * SPAN : (high - first) * SPAN]
                back = jnp.dot(taken, seen, preferred_element_type=F32).astype(BF16)
                back = back.reshape(EDGE, EDGE, frames)
                rows = slice(b * EDGE, (b + 1) * EDGE)
                if sweep == PASSES - 1:
                    backs[j, rows] = back
                errs[j, rows] = (pm[j, rows] + back.astype(F32)).astype(BF16)

        grad = lax.dot_general(
            foot[...].reshape(pixels, comps),
            errs[...].reshape(pixels, frames),
            (((0,), (0,)), ((), ())),
            preferred_element_type=F32,
        )
        for q in range(frames // LANES):
            cols = slice(q * LANES, (q + 1) * LANES)
            moved = jnp.maximum(trace[:, cols].astype(F32) - grad[:, cols] * inv_den[...], 0.0)
            trace[:, cols] = jnp.where(live, moved, 0.0).astype(BF16)

    trace_copy = pltpu.make_async_copy(trace, new_trace, out_sems.at[0])
    trace_copy.start()
    squares = jnp.zeros((comps, LANES), F32)
    for q in range(frames // LANES):
        now = trace[:, q * LANES : (q + 1) * LANES].astype(F32)
        squares = squares + now * now
    energy = jnp.sum(jnp.transpose(squares), axis=0, keepdims=True)
    energy_out[...] = energy

    def energy_copy(peer, sender):
        return pltpu.make_async_remote_copy(
            src_ref=energy_out,
            dst_ref=energy_in.at[sender],
            send_sem=energy_sems.at[0, peer],
            recv_sem=energy_sems.at[1, sender],
            device_id={"tm": peer},
            device_id_type=MESH,
        )

    def lines(share):
        return slice(bounds[share] * EDGE, bounds[share + 1] * EDGE)

    def part_copy(share, sender):
        return pltpu.make_async_remote_copy(
            src_ref=part.at[lines(share)],
            dst_ref=arrived.at[sender, 0 : (bounds[share + 1] - bounds[share]) * EDGE],
            send_sem=part_sems.at[0, share],
            recv_sem=part_sems.at[1, sender],
            device_id={"tm": share},
            device_id_type=MESH,
        )

    def gather_copy(peer, share):
        return pltpu.make_async_remote_copy(
            src_ref=gathered.at[lines(share)],
            dst_ref=gathered.at[lines(share)],
            send_sem=gather_sems.at[0, peer],
            recv_sem=gather_sems.at[1, share],
            device_id={"tm": peer},
            device_id_type=MESH,
        )

    def over_peers(do):
        def step(t, carry):
            do(lax.rem(me + 1 + t, n))
            return carry

        lax.fori_loop(0, n - 1, step, 0)

    over_peers(lambda peer: energy_copy(peer, me).start())

    def rows_of(ref, runs):
        found = jnp.concatenate([ref[j, low:high] for j, low, high, _ in runs], axis=0)
        return found.reshape(found.shape[0] * EDGE, ref.shape[3])

    def fold(values, runs, first, last):
        values = values.reshape(-1, EDGE, comps)
        totals, at = [None] * (last - first), 0
        for _, low, high, row in runs:
            for index in range(row - first, row - first + high - low):
                totals[index] = values[at] if totals[index] is None else totals[index] + values[at]
                at += 1
        return totals

    def grads_of(first, last):
        runs = fold_runs(first, last)
        feet = rows_of(foot, runs)
        prod = jnp.dot(feet, trace[...], preferred_element_type=F32)
        ferr = prod + rows_of(backs, runs).astype(F32) - rows_of(movie, runs).astype(F32)
        grad = lax.dot_general(
            ferr.astype(BF16), trace[...], (((1,), (1,)), ((), ())), preferred_element_type=F32
        )
        return fold(jnp.where(feet.astype(F32) > 0.0, grad, 0.0), runs, first, last)

    owned = [share for share in range(n) if bounds[share] < bounds[share + 1]]
    teams = share_teams(bounds)
    for team in teams[::ORDER]:
        first, last = bounds[team[0]], bounds[team[-1] + 1]
        found = grads_of(first, last)
        for index in range(last - first):
            part[(first + index) * EDGE : (first + index + 1) * EDGE] = found[index].astype(BF16)
        for share in team:
            @pl.when(me != share)
            def _():
                part_copy(share, me).start()

            @pl.when(me == share)
            def _():
                for row in range(bounds[share], bounds[share + 1]):
                    at = (row - bounds[share]) * EDGE
                    own[at : at + EDGE] = found[row - first]

    energy_in[me] = energy_out[...]

    def take_energy(peer):
        energy_copy(me, peer).wait_recv()
        energy_in[me] += energy_in[peer]

    over_peers(take_energy)
    den_c = energy_in[me] + RIDGE_TERM

    def settle(share):
        first, last = bounds[share], bounds[share + 1]
        size = (last - first) * EDGE

        def take(peer):
            part_copy(share, peer).wait_recv()
            own[0:size] += arrived[peer, 0:size].astype(F32)

        over_peers(take)
        runs = fold_runs(first, last)
        feet = jnp.concatenate(fold(rows_of(foot, runs).astype(F32), runs, first, last), axis=0)
        gathered[lines(share)] = jnp.maximum(feet - own[0:size] / den_c, 0.0).astype(BF16)
        over_peers(lambda peer: gather_copy(peer, share).start())

    for share in owned:
        pl.when(me == share)(functools.partial(settle, share))
    for share in owned[::ORDER]:
        pl.when(me != share)(lambda: gather_copy(me, share).wait_recv())
    packed_copy = pltpu.make_async_copy(gathered, packed, out_sems.at[1])
    packed_copy.start()

    for sweep in range(PASSES):
        halo_copy(sweep).wait_send()

    over_peers(lambda peer: energy_copy(peer, me).wait_send())
    for share in owned:
        pl.when(me != share)(lambda: part_copy(share, me).wait_send())
        pl.when(me == share)(lambda: over_peers(lambda peer: gather_copy(peer, share).wait_send()))
    trace_copy.wait()
    packed_copy.wait()


def unfold(
    packed_in, trace_in, row_in, col_in, reach_in, count,
    new_foot, new_trace,
    packed, trace, row_at, col_at, reach, values, feet, load_sems, foot_sems,
):
    comps = feet.shape[2]
    loads = [
        pltpu.make_async_copy(source, target, load_sems.at[index])
        for index, (source, target) in enumerate((
            (packed_in, packed), (trace_in, trace), (row_in, row_at), (col_in, col_at), (reach_in, reach),
        ))
    ]
    for copy in loads:
        copy.start()
    for index in (0, 2, 3, 4):
        loads[index].wait()
    live = lax.broadcasted_iota(jnp.int32, (1, comps), 1) < count[0]
    bound = jnp.where(live, reach[...] * reach[...], -1)
    for r in range(FOLD_ROWS):
        values[r] = packed[r * EDGE : (r + 1) * EDGE].astype(F32)
    loads[1].wait()
    trace_copy = pltpu.make_async_copy(trace, new_trace, load_sems.at[1])
    trace_copy.start()
    col_sq = []
    for j in range(TILES):
        gap = lax.broadcasted_iota(jnp.int32, (EDGE, comps), 0) + j * EDGE - col_at[...]
        col_sq.append(gap * gap)

    def row(r):
        row_gap = r - row_at[...]
        edge = bound - row_gap * row_gap
        for j in range(TILES):
            value = values[lax.rem(r + (FOLD_ROWS - SHIFT) * j, FOLD_ROWS)]
            feet[r, j * EDGE : (j + 1) * EDGE] = jnp.where(col_sq[j] <= edge, value, 0.0).astype(BF16)

    copies = []
    for b in range(TILES):
        def step(t, carry):
            for u in range(2):
                row(b * EDGE + t * 2 + u)
            return carry

        lax.fori_loop(0, EDGE // 2, step, 0)
        rows = slice(b * EDGE, (b + 1) * EDGE)
        copies.append(pltpu.make_async_copy(feet.at[rows], new_foot.at[rows], foot_sems.at[b]))
        copies[-1].start()
    for copy in copies:
        copy.wait()
    trace_copy.wait()


def shards(movie, cycle_weights, footprints, traces, centre_row, centre_col, radius, comp_count):
    n = lax.axis_size("tm")
    frames = movie.shape[2]
    comps = footprints.shape[2]
    taps = cycle_weights.shape[2]
    bounds = share_bounds(n)
    widest = max(high - low for low, high in zip(bounds, bounds[1:])) * EDGE
    anyspace = pl.BlockSpec(memory_space=pl.ANY)
    smem = pl.BlockSpec(memory_space=pltpu.SMEM)
    dma = pltpu.SemaphoreType.DMA
    packed, trace = pl.pallas_call(
        functools.partial(kernel, n, bounds),
        out_shape=(
            jax.ShapeDtypeStruct((FOLD_ROWS * EDGE, comps), BF16),
            jax.ShapeDtypeStruct((comps, frames), BF16),
        ),
        in_specs=[anyspace] * 7 + [smem, anyspace],
        out_specs=(anyspace, anyspace),
        scratch_shapes=[
            pltpu.VMEM((TILES, SIDE, EDGE, frames), BF16),
            pltpu.VMEM((taps, SIDE * SIDE), BF16),
            pltpu.VMEM((TILES, SIDE, EDGE, comps), BF16),
            pltpu.VMEM((comps, frames), BF16),
            pltpu.VMEM((1, comps), jnp.int32),
            pltpu.VMEM((1, comps), jnp.int32),
            pltpu.VMEM((1, comps), jnp.int32),
            pltpu.VMEM((STEP, CHUNKS, EDGE, LANES), jnp.int16),
            pltpu.VMEM((SIDE, TILES, EDGE, LANES), BF16),
            pltpu.VMEM((TILES, SIDE, EDGE, comps), BF16),
            pltpu.VMEM((TILES, TILES, EDGE * EDGE, SPAN * SPAN), BF16),
            pltpu.VMEM((TILES, SIDE, EDGE, frames), F32),
            pltpu.VMEM((PASSES, SIDE, TILES + 1, EDGE, frames), BF16),
            pltpu.VMEM((TILES, SIDE, EDGE, frames), BF16),
            pltpu.VMEM((TILES, SIDE, EDGE, frames), BF16),
            pltpu.VMEM((comps, LANES), F32),
            pltpu.VMEM((PASSES, SIDE * CYCLE, frames), BF16),
            pltpu.VMEM((PASSES, SIDE * CYCLE, frames), BF16),
            pltpu.VMEM((FOLD_ROWS * EDGE, comps), BF16),
            pltpu.VMEM((widest, comps), F32),
            pltpu.VMEM((n, widest, comps), BF16),
            pltpu.VMEM((1, comps), F32),
            pltpu.VMEM((n, 1, comps), F32),
            pltpu.VMEM((FOLD_ROWS * EDGE, comps), BF16),
            dma((2, TILES, TILES)),
            dma((6,)),
            dma((2, PASSES)),
            dma((2, n)),
            dma((2, n)),
            dma((2, n)),
            dma((2,)),
        ],
        compiler_params=pltpu.CompilerParams(
            collective_id=0, has_side_effects=True, vmem_limit_bytes=60 * 1024 * 1024
        ),
    )(
        movie.reshape(SIDE, SIDE, frames),
        jnp.transpose(cycle_weights[0]),
        footprints.reshape(SIDE, SIDE, comps),
        traces.reshape(comps, frames),
        centre_row,
        centre_col,
        radius,
        comp_count,
        jnp.asarray(tap_tables()),
    )
    new_foot, new_trace = pl.pallas_call(
        unfold,
        out_shape=(
            jax.ShapeDtypeStruct((SIDE, SIDE, comps), BF16),
            jax.ShapeDtypeStruct((comps, frames), BF16),
        ),
        in_specs=[anyspace] * 5 + [smem],
        out_specs=(anyspace, anyspace),
        scratch_shapes=[
            pltpu.VMEM((FOLD_ROWS * EDGE, comps), BF16),
            pltpu.VMEM((comps, frames), BF16),
            pltpu.VMEM((1, comps), jnp.int32),
            pltpu.VMEM((1, comps), jnp.int32),
            pltpu.VMEM((1, comps), jnp.int32),
            pltpu.VMEM((FOLD_ROWS, EDGE, comps), F32),
            pltpu.VMEM((SIDE, SIDE, comps), BF16),
            dma((5,)),
            dma((TILES,)),
        ],
    )(packed, trace, centre_row, centre_col, radius, comp_count)
    return (new_foot.reshape(1, SIDE * SIDE, comps), new_trace[None])


def solution(mesh):
    in_specs = (
        P(("groups", "tile"), None, "tm"),
        P(("groups", "tile"), None, None),
        P(("groups", "tile"), None, None),
        P(("groups", "tile"), None, "tm"),
        P(("groups", "tile"), None),
        P(("groups", "tile"), None),
        P(("groups", "tile"), None),
        P(("groups", "tile")),
    )
    out_specs = (P(("groups", "tile"), None, None), P(("groups", "tile"), None, "tm"))
    return jax.shard_map(shards, mesh=mesh, in_specs=in_specs, out_specs=out_specs, check_vma=False)
```

```python
import functools

import jax
import jax.numpy as jnp
import numpy as np
from jax import lax
from jax.experimental import pallas as pl
from jax.experimental.pallas import tpu as pltpu
from jax.sharding import PartitionSpec as P

SIDE = 48
CYCLE = 8
PASSES = 2
RIDGE_TERM = 1.0
EDGE = 16
TILES = SIDE // EDGE
SPAN = EDGE + 2 * CYCLE
LANES = 128
STEP = LANES // SPAN
CHUNKS = (STEP - 1 + 2 * CYCLE) // STEP + 1
FOLD_ROWS = 19
SHIFT = 9
TEAM_ROWS = 4
ORDER = -1
F32 = jnp.float32
BF16 = jnp.bfloat16
MESH = pl.DeviceIdType.MESH


def cycle_offsets():
    found = []
    for row_step in range(-CYCLE, CYCLE + 1):
        for col_step in range(-CYCLE, CYCLE + 1):
            dist_sq = row_step * row_step + col_step * col_step
            if CYCLE * CYCLE <= dist_sq < (CYCLE + 1) * (CYCLE + 1):
                found.append((row_step, col_step))
    return found


def tap_tables():
    offsets = {step: index for index, step in enumerate(cycle_offsets())}
    tables = np.full((STEP, CHUNKS, EDGE, LANES), len(offsets), np.int16)
    for phase in range(STEP):
        for chunk in range(CHUNKS):
            for col in range(EDGE):
                for lane in range(LANES):
                    row_step = chunk * STEP + lane // SPAN - phase - CYCLE
                    col_step = lane % SPAN - col - CYCLE
                    if (row_step, col_step) in offsets:
                        tables[phase, chunk, col, lane] = offsets[(row_step, col_step)]
    return tables


def share_bounds(n):
    base, extra = divmod(FOLD_ROWS, n)
    bounds = [0]
    for index in range(n):
        bounds.append(bounds[-1] + base + (index >= n - extra))
    return bounds


def share_teams(bounds):
    teams, held = [], []
    for share in range(len(bounds) - 1):
        if bounds[share] < bounds[share + 1]:
            held.append(share)
        if held and bounds[share + 1] - bounds[held[0]] >= TEAM_ROWS:
            teams.append(held)
            held = []
    return teams + [held] if held else teams


def fold_runs(first, last):
    runs = []
    for j in range(TILES):
        for lap in range(-TILES, TILES + 1):
            moved = SHIFT * j + FOLD_ROWS * lap
            low, high = max(first + moved, 0), min(last + moved, SIDE)
            if low < high:
                runs.append((j, low, high, low - moved))
    return runs


def pick(values, index):
    numbers = lax.GatherDimensionNumbers(
        offset_dims=(), collapsed_slice_dims=(1,), start_index_map=(1,),
        operand_batching_dims=(0,), start_indices_batching_dims=(0,),
    )
    inside = lax.GatherScatterMode.PROMISE_IN_BOUNDS
    return lax.gather(values, index[..., None], numbers, (1, 1), mode=inside)


def kernel(
    n, bounds,
    movie_in, stored_in, prints_in, traces_in, row_in, col_in, reach_in, count, tables_in,
    packed, new_trace,
    movie, stored, prints, trace, row_at, col_at, reach, tables,
    weights, foot, band_first, band_second, band_third, pm, win, errs, backs, inv_den,
    halo_out, halo_in, part, own, arrived, energy_out, energy_in, gathered,
    load_sems, small_sems, halo_sems, part_sems, energy_sems, gather_sems, out_sems,
):
    me = lax.axis_index("tm")
    tile = lax.axis_index("tile")
    frames = movie.shape[3]
    comps = foot.shape[3]
    pixels = SIDE * SIDE

    def load(b, j, kind):
        source, target = ((prints_in, prints), (movie_in, movie))[kind]
        rows = slice(b * EDGE, (b + 1) * EDGE)
        return pltpu.make_async_copy(
            source.at[rows, j * EDGE : (j + 1) * EDGE], target.at[j, rows], load_sems.at[kind, b, j]
        )

    smalls = [
        pltpu.make_async_copy(source, target, small_sems.at[index])
        for index, (source, target) in enumerate((
            (row_in, row_at), (col_in, col_at), (reach_in, reach),
            (stored_in, stored), (tables_in, tables), (traces_in, trace),
        ))
    ]
    for copy in smalls:
        copy.start()
    for b in range(TILES):
        for kind in range(2):
            for j in range(TILES):
                load(b, j, kind).start()

    barrier = pltpu.get_barrier_semaphore()
    pl.semaphore_signal(barrier, inc=1, device_id={"tile": 1 - tile}, device_id_type=MESH)

    def greet(t, carry):
        peer = lax.rem(me + 1 + t, n)
        pl.semaphore_signal(barrier, inc=1, device_id={"tm": peer}, device_id_type=MESH)
        return carry

    lax.fori_loop(0, n - 1, greet, 0)

    blank = jnp.zeros((SIDE, CYCLE, frames), BF16)
    for sweep in range(PASSES):
        win[sweep, :, 0, 0:CYCLE] = blank
        win[sweep, :, TILES, CYCLE:EDGE] = blank

    for copy in smalls:
        copy.wait()
    live_row = lax.broadcasted_iota(jnp.int32, (1, comps), 1) < count[0]
    bound = jnp.where(live_row, reach[...] * reach[...], -1)
    live = lax.broadcasted_iota(jnp.int32, (comps, LANES), 0) < count[0]
    for q in range(frames // LANES):
        cols = slice(q * LANES, (q + 1) * LANES)
        trace[:, cols] = jnp.where(live, trace[:, cols].astype(F32), 0.0).astype(BF16)

    col_sq = []
    for j in range(TILES):
        gap = lax.broadcasted_iota(jnp.int32, (EDGE, comps), 0) + j * EDGE - col_at[...]
        col_sq.append(gap * gap)

    def store_window(sweep, rows, j, diff):
        resid = (-diff).astype(BF16)
        win[sweep, rows, j, CYCLE:EDGE] = resid[:, 0:CYCLE]
        win[sweep, rows, j + 1, 0:CYCLE] = resid[:, CYCLE:EDGE]

    near = [jnp.where(tile == 0, TILES - 1 - t, t) for t in range(TILES)]
    bands = (band_first, band_second, band_third)

    def weave(t, b, q, phase):
        spot = (q * STEP + phase) * EDGE
        held = weights[b * EDGE + q * STEP + phase, near[TILES - 1 - t]]
        for chunk in range(SPAN // STEP):
            if isinstance(q, int):
                rows, lane = slice(spot, spot + EDGE), (q + chunk) % (SPAN // STEP) * LANES
                lanes = slice(lane, lane + LANES)
            else:
                rows = pl.ds(pl.multiple_of(spot, EDGE), EDGE)
                lane = q + chunk if chunk < CHUNKS else lax.rem(q + chunk, SPAN // STEP)
                lanes = pl.ds(pl.multiple_of(lane * LANES, LANES), LANES)
            if chunk < CHUNKS:
                bands[t][b, rows, lanes] = pick(held, tables[phase, chunk])
            else:
                bands[t][b, rows, lanes] = jnp.zeros((EDGE, LANES), BF16)

    def wait_for(kind, b):
        for j in range(TILES):
            load(b, j, kind).wait()

    def mask_rows(b, total):
        for r in range(b * EDGE, (b + 1) * EDGE):
            row_gap = r - row_at[...]
            edge = bound - row_gap * row_gap
            for j in range(TILES):
                kept = jnp.where(col_sq[j] <= edge, prints[j, r].astype(F32), 0.0)
                foot[j, r] = kept.astype(BF16)
                total = total + kept * kept
        return total

    def first_residual(b):
        rows = slice(b * EDGE, (b + 1) * EDGE)
        feet = foot[:, rows].reshape(TILES * EDGE * EDGE, comps)
        prod = jnp.dot(feet, trace[...], preferred_element_type=F32)
        prod = prod.reshape(TILES, EDGE, EDGE, frames)
        for j in range(TILES):
            diff = prod[j] - movie[j, rows].astype(F32)
            pm[j, rows] = diff
            store_window(0, rows, j, diff)

    taps = stored.shape[0]
    run = CYCLE * SIDE
    for h in range(SIDE // CYCLE):
        values = stored[:, h * run : (h + 1) * run].astype(F32)
        values = jnp.concatenate([values, jnp.zeros((LANES - taps, run), F32)], axis=0)
        turned = jnp.transpose(values).astype(BF16)
        weights[h * CYCLE : (h + 1) * CYCLE] = turned.reshape(CYCLE, TILES, EDGE, LANES)
    wait_for(0, 0)
    total = mask_rows(0, jnp.zeros((EDGE, comps), F32))
    for b in range(TILES):
        wait_for(1, b)
        if b + 1 < TILES:
            wait_for(0, b + 1)
            total = mask_rows(b + 1, total)
        first_residual(b)
        for i in range(EDGE):
            weave(0, b, i // STEP, i % STEP)
    den = jnp.sum(total, axis=0, keepdims=True) + RIDGE_TERM
    inv_den[...] = jnp.transpose(jnp.broadcast_to(1.0 / den, (LANES, comps)))

    def halo_copy(sweep):
        return pltpu.make_async_remote_copy(
            src_ref=halo_out.at[sweep],
            dst_ref=halo_in.at[sweep],
            send_sem=halo_sems.at[0, sweep],
            recv_sem=halo_sems.at[1, sweep],
            device_id={"tile": 1 - tile},
            device_id_type=MESH,
        )

    def send_halo(sweep, diff):
        cut = jnp.where(tile == 0, diff[:, CYCLE:EDGE], diff[:, 0:CYCLE])
        halo_out[sweep] = (-cut).reshape(SIDE * CYCLE, frames).astype(BF16)
        halo_copy(sweep).start()

    for sweep in range(PASSES):
        if sweep == 0:
            pl.semaphore_wait(barrier, n)
            send_halo(0, pm[near[0]])
        else:
            for t in range(TILES):
                j = near[t]
                prod = jnp.dot(
                    foot[j].reshape(SIDE * EDGE, comps), trace[...], preferred_element_type=F32
                )
                diff = prod.reshape(SIDE, EDGE, frames) - movie[j].astype(F32)
                pm[j] = diff
                store_window(sweep, slice(0, SIDE), j, diff)
                if t == 0:
                    send_halo(sweep, diff)

        for t in range(TILES):
            j = near[TILES - 1 - t]
            if t == TILES - 1:
                halo_copy(sweep).wait_recv()
                came = halo_in[sweep].astype(F32).reshape(SIDE, CYCLE, frames).astype(BF16)

                @pl.when(tile == 0)
                def _():
                    win[sweep, :, TILES, CYCLE:EDGE] = came

                @pl.when(tile != 0)
                def _():
                    win[sweep, :, 0, 0:CYCLE] = came

            for b in range(TILES):
                if sweep == 0 and t + 1 < TILES:
                    for i in range(EDGE):
                        weave(t + 1, b, i // STEP, i % STEP)
                first = b * EDGE - CYCLE
                low, high = max(first, 0), min(first + SPAN, SIDE)
                seen = win[sweep, low:high, pl.ds(j, 2)].reshape((high - low) * SPAN, frames)
                taken = bands[t][b, :, (low - first) * SPAN : (high - first) * SPAN]
                back = jnp.dot(taken, seen, preferred_element_type=F32).astype(BF16)
                back = back.reshape(EDGE, EDGE, frames)
                rows = slice(b * EDGE, (b + 1) * EDGE)
                if sweep == PASSES - 1:
                    backs[j, rows] = back
                errs[j, rows] = (pm[j, rows] + back.astype(F32)).astype(BF16)

        grad = lax.dot_general(
            foot[...].reshape(pixels, comps),
            errs[...].reshape(pixels, frames),
            (((0,), (0,)), ((), ())),
            preferred_element_type=F32,
        )
        for q in range(frames // LANES):
            cols = slice(q * LANES, (q + 1) * LANES)
            moved = jnp.maximum(trace[:, cols].astype(F32) - grad[:, cols] * inv_den[...], 0.0)
            trace[:, cols] = jnp.where(live, moved, 0.0).astype(BF16)

    trace_copy = pltpu.make_async_copy(trace, new_trace, out_sems.at[0])
    trace_copy.start()
    squares = jnp.zeros((comps, LANES), F32)
    for q in range(frames // LANES):
        now = trace[:, q * LANES : (q + 1) * LANES].astype(F32)
        squares = squares + now * now
    energy = jnp.sum(jnp.transpose(squares), axis=0, keepdims=True)
    energy_out[...] = energy

    def energy_copy(peer, sender):
        return pltpu.make_async_remote_copy(
            src_ref=energy_out,
            dst_ref=energy_in.at[sender],
            send_sem=energy_sems.at[0, peer],
            recv_sem=energy_sems.at[1, sender],
            device_id={"tm": peer},
            device_id_type=MESH,
        )

    def lines(share):
        return slice(bounds[share] * EDGE, bounds[share + 1] * EDGE)

    def part_copy(share, sender):
        return pltpu.make_async_remote_copy(
            src_ref=part.at[lines(share)],
            dst_ref=arrived.at[sender, 0 : (bounds[share + 1] - bounds[share]) * EDGE],
            send_sem=part_sems.at[0, share],
            recv_sem=part_sems.at[1, sender],
            device_id={"tm": share},
            device_id_type=MESH,
        )

    def gather_copy(peer, share):
        return pltpu.make_async_remote_copy(
            src_ref=gathered.at[lines(share)],
            dst_ref=gathered.at[lines(share)],
            send_sem=gather_sems.at[0, peer],
            recv_sem=gather_sems.at[1, share],
            device_id={"tm": peer},
            device_id_type=MESH,
        )

    def over_peers(do):
        def step(t, carry):
            do(lax.rem(me + 1 + t, n))
            return carry

        lax.fori_loop(0, n - 1, step, 0)

    over_peers(lambda peer: energy_copy(peer, me).start())

    def rows_of(ref, runs):
        found = jnp.concatenate([ref[j, low:high] for j, low, high, _ in runs], axis=0)
        return found.reshape(found.shape[0] * EDGE, ref.shape[3])

    def fold(values, runs, first, last):
        values = values.reshape(-1, EDGE, comps)
        totals, at = [None] * (last - first), 0
        for _, low, high, row in runs:
            for index in range(row - first, row - first + high - low):
                totals[index] = values[at] if totals[index] is None else totals[index] + values[at]
                at += 1
        return totals

    def grads_of(first, last):
        runs = fold_runs(first, last)
        feet = rows_of(foot, runs)
        prod = jnp.dot(feet, trace[...], preferred_element_type=F32)
        ferr = prod + rows_of(backs, runs).astype(F32) - rows_of(movie, runs).astype(F32)
        grad = lax.dot_general(
            ferr.astype(BF16), trace[...], (((1,), (1,)), ((), ())), preferred_element_type=F32
        )
        return fold(jnp.where(feet.astype(F32) > 0.0, grad, 0.0), runs, first, last)

    owned = [share for share in range(n) if bounds[share] < bounds[share + 1]]
    teams = share_teams(bounds)
    for team in teams[::ORDER]:
        first, last = bounds[team[0]], bounds[team[-1] + 1]
        found = grads_of(first, last)
        for index in range(last - first):
            part[(first + index) * EDGE : (first + index + 1) * EDGE] = found[index].astype(BF16)
        for share in team:
            @pl.when(me != share)
            def _():
                part_copy(share, me).start()

            @pl.when(me == share)
            def _():
                for row in range(bounds[share], bounds[share + 1]):
                    at = (row - bounds[share]) * EDGE
                    own[at : at + EDGE] = found[row - first]

    energy_in[me] = energy_out[...]

    def take_energy(peer):
        energy_copy(me, peer).wait_recv()
        energy_in[me] += energy_in[peer]

    over_peers(take_energy)
    den_c = energy_in[me] + RIDGE_TERM

    def settle(share):
        first, last = bounds[share], bounds[share + 1]
        size = (last - first) * EDGE

        def take(peer):
            part_copy(share, peer).wait_recv()
            own[0:size] += arrived[peer, 0:size].astype(F32)

        over_peers(take)
        runs = fold_runs(first, last)
        feet = jnp.concatenate(fold(rows_of(foot, runs).astype(F32), runs, first, last), axis=0)
        gathered[lines(share)] = jnp.maximum(feet - own[0:size] / den_c, 0.0).astype(BF16)
        over_peers(lambda peer: gather_copy(peer, share).start())

    for share in owned:
        pl.when(me == share)(functools.partial(settle, share))
    for share in owned[::ORDER]:
        pl.when(me != share)(lambda: gather_copy(me, share).wait_recv())
    packed_copy = pltpu.make_async_copy(gathered, packed, out_sems.at[1])
    packed_copy.start()

    for sweep in range(PASSES):
        halo_copy(sweep).wait_send()

    over_peers(lambda peer: energy_copy(peer, me).wait_send())
    for share in owned:
        pl.when(me != share)(lambda: part_copy(share, me).wait_send())
        pl.when(me == share)(lambda: over_peers(lambda peer: gather_copy(peer, share).wait_send()))
    trace_copy.wait()
    packed_copy.wait()


def unfold(
    packed_in, trace_in, row_in, col_in, reach_in, count,
    new_foot, new_trace,
    packed, trace, row_at, col_at, reach, values, feet, load_sems, foot_sems,
):
    comps = feet.shape[2]
    loads = [
        pltpu.make_async_copy(source, target, load_sems.at[index])
        for index, (source, target) in enumerate((
            (packed_in, packed), (trace_in, trace), (row_in, row_at), (col_in, col_at), (reach_in, reach),
        ))
    ]
    for copy in loads:
        copy.start()
    for index in (0, 2, 3, 4):
        loads[index].wait()
    live = lax.broadcasted_iota(jnp.int32, (1, comps), 1) < count[0]
    bound = jnp.where(live, reach[...] * reach[...], -1)
    for r in range(FOLD_ROWS):
        values[r] = packed[r * EDGE : (r + 1) * EDGE].astype(F32)
    loads[1].wait()
    trace_copy = pltpu.make_async_copy(trace, new_trace, load_sems.at[1])
    trace_copy.start()
    col_sq = []
    for j in range(TILES):
        gap = lax.broadcasted_iota(jnp.int32, (EDGE, comps), 0) + j * EDGE - col_at[...]
        col_sq.append(gap * gap)

    def row(r):
        row_gap = r - row_at[...]
        edge = bound - row_gap * row_gap
        for j in range(TILES):
            value = values[lax.rem(r + (FOLD_ROWS - SHIFT) * j, FOLD_ROWS)]
            feet[r, j * EDGE : (j + 1) * EDGE] = jnp.where(col_sq[j] <= edge, value, 0.0).astype(BF16)

    copies = []
    for b in range(SIDE // CYCLE):
        def step(t, carry):
            for u in range(4):
                row(b * CYCLE + t * 4 + u)
            return carry

        lax.fori_loop(0, CYCLE // 4, step, 0)
        rows = slice(b * CYCLE, (b + 1) * CYCLE)
        copies.append(pltpu.make_async_copy(feet.at[rows], new_foot.at[rows], foot_sems.at[b]))
        copies[-1].start()
    for copy in copies:
        copy.wait()
    trace_copy.wait()


def shards(movie, cycle_weights, footprints, traces, centre_row, centre_col, radius, comp_count):
    n = lax.axis_size("tm")
    frames = movie.shape[2]
    comps = footprints.shape[2]
    taps = cycle_weights.shape[2]
    bounds = share_bounds(n)
    widest = max(high - low for low, high in zip(bounds, bounds[1:])) * EDGE
    anyspace = pl.BlockSpec(memory_space=pl.ANY)
    smem = pl.BlockSpec(memory_space=pltpu.SMEM)
    dma = pltpu.SemaphoreType.DMA
    packed, trace = pl.pallas_call(
        functools.partial(kernel, n, bounds),
        out_shape=(
            jax.ShapeDtypeStruct((FOLD_ROWS * EDGE, comps), BF16),
            jax.ShapeDtypeStruct((comps, frames), BF16),
        ),
        in_specs=[anyspace] * 7 + [smem, anyspace],
        out_specs=(anyspace, anyspace),
        scratch_shapes=[
            pltpu.VMEM((TILES, SIDE, EDGE, frames), BF16),
            pltpu.VMEM((taps, SIDE * SIDE), BF16),
            pltpu.VMEM((TILES, SIDE, EDGE, comps), BF16),
            pltpu.VMEM((comps, frames), BF16),
            pltpu.VMEM((1, comps), jnp.int32),
            pltpu.VMEM((1, comps), jnp.int32),
            pltpu.VMEM((1, comps), jnp.int32),
            pltpu.VMEM((STEP, CHUNKS, EDGE, LANES), jnp.int16),
            pltpu.VMEM((SIDE, TILES, EDGE, LANES), BF16),
            pltpu.VMEM((TILES, SIDE, EDGE, comps), BF16),
            pltpu.VMEM((TILES, EDGE * EDGE, SPAN * SPAN), BF16),
            pltpu.VMEM((TILES, EDGE * EDGE, SPAN * SPAN), BF16),
            pltpu.VMEM((TILES, EDGE * EDGE, SPAN * SPAN), BF16),
            pltpu.VMEM((TILES, SIDE, EDGE, frames), F32),
            pltpu.VMEM((PASSES, SIDE, TILES + 1, EDGE, frames), BF16),
            pltpu.VMEM((TILES, SIDE, EDGE, frames), BF16),
            pltpu.VMEM((TILES, SIDE, EDGE, frames), BF16),
            pltpu.VMEM((comps, LANES), F32),
            pltpu.VMEM((PASSES, SIDE * CYCLE, frames), BF16),
            pltpu.VMEM((PASSES, SIDE * CYCLE, frames), BF16),
            pltpu.VMEM((FOLD_ROWS * EDGE, comps), BF16),
            pltpu.VMEM((widest, comps), F32),
            pltpu.VMEM((n, widest, comps), BF16),
            pltpu.VMEM((1, comps), F32),
            pltpu.VMEM((n, 1, comps), F32),
            pltpu.VMEM((FOLD_ROWS * EDGE, comps), BF16),
            dma((2, TILES, TILES)),
            dma((6,)),
            dma((2, PASSES)),
            dma((2, n)),
            dma((2, n)),
            dma((2, n)),
            dma((2,)),
        ],
        compiler_params=pltpu.CompilerParams(
            collective_id=0, has_side_effects=True, vmem_limit_bytes=60 * 1024 * 1024
        ),
    )(
        movie.reshape(SIDE, SIDE, frames),
        jnp.transpose(cycle_weights[0]),
        footprints.reshape(SIDE, SIDE, comps),
        traces.reshape(comps, frames),
        centre_row,
        centre_col,
        radius,
        comp_count,
        jnp.asarray(tap_tables()),
    )
    new_foot, new_trace = pl.pallas_call(
        unfold,
        out_shape=(
            jax.ShapeDtypeStruct((SIDE, SIDE, comps), BF16),
            jax.ShapeDtypeStruct((comps, frames), BF16),
        ),
        in_specs=[anyspace] * 5 + [smem],
        out_specs=(anyspace, anyspace),
        scratch_shapes=[
            pltpu.VMEM((FOLD_ROWS * EDGE, comps), BF16),
            pltpu.VMEM((comps, frames), BF16),
            pltpu.VMEM((1, comps), jnp.int32),
            pltpu.VMEM((1, comps), jnp.int32),
            pltpu.VMEM((1, comps), jnp.int32),
            pltpu.VMEM((FOLD_ROWS, EDGE, comps), F32),
            pltpu.VMEM((SIDE, SIDE, comps), BF16),
            dma((5,)),
            dma((SIDE // CYCLE,)),
        ],
    )(packed, trace, centre_row, centre_col, radius, comp_count)
    return (new_foot.reshape(1, SIDE * SIDE, comps), new_trace[None])


def solution(mesh):
    in_specs = (
        P(("groups", "tile"), None, "tm"),
        P(("groups", "tile"), None, None),
        P(("groups", "tile"), None, None),
        P(("groups", "tile"), None, "tm"),
        P(("groups", "tile"), None),
        P(("groups", "tile"), None),
        P(("groups", "tile"), None),
        P(("groups", "tile")),
    )
    out_specs = (P(("groups", "tile"), None, None), P(("groups", "tile"), None, "tm"))
    return jax.shard_map(shards, mesh=mesh, in_specs=in_specs, out_specs=out_specs, check_vma=False)
```

```python
import functools

import jax
import jax.numpy as jnp
import numpy as np
from jax import lax
from jax.experimental import pallas as pl
from jax.experimental.pallas import tpu as pltpu
from jax.sharding import PartitionSpec as P

SIDE = 48
CYCLE = 8
PASSES = 2
RIDGE_TERM = 1.0
EDGE = 16
TILES = SIDE // EDGE
SPAN = EDGE + 2 * CYCLE
LANES = 128
STEP = LANES // SPAN
CHUNKS = (STEP - 1 + 2 * CYCLE) // STEP + 1
FOLD_ROWS = 19
SHIFT = 9
TEAM_ROWS = 4
ORDER = -1
F32 = jnp.float32
BF16 = jnp.bfloat16
MESH = pl.DeviceIdType.MESH


def cycle_offsets():
    found = []
    for row_step in range(-CYCLE, CYCLE + 1):
        for col_step in range(-CYCLE, CYCLE + 1):
            dist_sq = row_step * row_step + col_step * col_step
            if CYCLE * CYCLE <= dist_sq < (CYCLE + 1) * (CYCLE + 1):
                found.append((row_step, col_step))
    return found


def tap_tables():
    offsets = {step: index for index, step in enumerate(cycle_offsets())}
    tables = np.full((STEP, CHUNKS, EDGE, LANES), len(offsets), np.int16)
    for phase in range(STEP):
        for chunk in range(CHUNKS):
            for col in range(EDGE):
                for lane in range(LANES):
                    row_step = chunk * STEP + lane // SPAN - phase - CYCLE
                    col_step = lane % SPAN - col - CYCLE
                    if (row_step, col_step) in offsets:
                        tables[phase, chunk, col, lane] = offsets[(row_step, col_step)]
    return tables


def share_bounds(n):
    base, extra = divmod(FOLD_ROWS, n)
    bounds = [0]
    for index in range(n):
        bounds.append(bounds[-1] + base + (index >= n - extra))
    return bounds


def share_teams(bounds):
    teams, held = [], []
    for share in range(len(bounds) - 1):
        if bounds[share] < bounds[share + 1]:
            held.append(share)
        if held and bounds[share + 1] - bounds[held[0]] >= TEAM_ROWS:
            teams.append(held)
            held = []
    return teams + [held] if held else teams


def fold_runs(first, last):
    runs = []
    for j in range(TILES):
        for lap in range(-TILES, TILES + 1):
            moved = SHIFT * j + FOLD_ROWS * lap
            low, high = max(first + moved, 0), min(last + moved, SIDE)
            if low < high:
                runs.append((j, low, high, low - moved))
    return runs


def pick(values, index):
    numbers = lax.GatherDimensionNumbers(
        offset_dims=(), collapsed_slice_dims=(1,), start_index_map=(1,),
        operand_batching_dims=(0,), start_indices_batching_dims=(0,),
    )
    inside = lax.GatherScatterMode.PROMISE_IN_BOUNDS
    return lax.gather(values, index[..., None], numbers, (1, 1), mode=inside)


def kernel(
    n, bounds,
    movie_in, stored_in, prints_in, traces_in, row_in, col_in, reach_in, count, tables_in,
    packed, new_trace,
    movie, stored, prints, trace, row_at, col_at, reach, tables,
    weights, foot, band_first, band_second, band_third, pm, win, errs, backs, inv_den,
    halo_out, halo_in, part, own, arrived, energy_out, energy_in, gathered,
    load_sems, small_sems, halo_sems, part_sems, energy_sems, gather_sems,
):
    me = lax.axis_index("tm")
    tile = lax.axis_index("tile")
    frames = movie.shape[3]
    comps = foot.shape[3]
    pixels = SIDE * SIDE

    def load(b, j, kind):
        source, target = ((prints_in, prints), (movie_in, movie))[kind]
        rows = slice(b * EDGE, (b + 1) * EDGE)
        return pltpu.make_async_copy(
            source.at[rows, j * EDGE : (j + 1) * EDGE], target.at[j, rows], load_sems.at[kind, b, j]
        )

    smalls = [
        pltpu.make_async_copy(source, target, small_sems.at[index])
        for index, (source, target) in enumerate((
            (row_in, row_at), (col_in, col_at), (reach_in, reach),
            (stored_in, stored), (tables_in, tables), (traces_in, trace),
        ))
    ]
    for copy in smalls:
        copy.start()
    for b in range(TILES):
        for kind in range(2):
            for j in range(TILES):
                load(b, j, kind).start()

    barrier = pltpu.get_barrier_semaphore()
    pl.semaphore_signal(barrier, inc=1, device_id={"tile": 1 - tile}, device_id_type=MESH)

    def greet(t, carry):
        peer = lax.rem(me + 1 + t, n)
        pl.semaphore_signal(barrier, inc=1, device_id={"tm": peer}, device_id_type=MESH)
        return carry

    lax.fori_loop(0, n - 1, greet, 0)

    blank = jnp.zeros((SIDE, CYCLE, frames), BF16)
    for sweep in range(PASSES):
        win[sweep, :, 0, 0:CYCLE] = blank
        win[sweep, :, TILES, CYCLE:EDGE] = blank

    for copy in smalls:
        copy.wait()
    live_row = lax.broadcasted_iota(jnp.int32, (1, comps), 1) < count[0]
    bound = jnp.where(live_row, reach[...] * reach[...], -1)
    live = lax.broadcasted_iota(jnp.int32, (comps, LANES), 0) < count[0]
    for q in range(frames // LANES):
        cols = slice(q * LANES, (q + 1) * LANES)
        trace[:, cols] = jnp.where(live, trace[:, cols].astype(F32), 0.0).astype(BF16)

    col_sq = []
    for j in range(TILES):
        gap = lax.broadcasted_iota(jnp.int32, (EDGE, comps), 0) + j * EDGE - col_at[...]
        col_sq.append(gap * gap)

    def store_window(sweep, rows, j, diff):
        resid = (-diff).astype(BF16)
        win[sweep, rows, j, CYCLE:EDGE] = resid[:, 0:CYCLE]
        win[sweep, rows, j + 1, 0:CYCLE] = resid[:, CYCLE:EDGE]

    near = [jnp.where(tile == 0, TILES - 1 - t, t) for t in range(TILES)]
    bands = (band_first, band_second, band_third)

    def weave(t, b, q, phase):
        spot = (q * STEP + phase) * EDGE
        held = weights[b * EDGE + q * STEP + phase, near[TILES - 1 - t]]
        for chunk in range(SPAN // STEP):
            if isinstance(q, int):
                rows, lane = slice(spot, spot + EDGE), (q + chunk) % (SPAN // STEP) * LANES
                lanes = slice(lane, lane + LANES)
            else:
                rows = pl.ds(pl.multiple_of(spot, EDGE), EDGE)
                lane = q + chunk if chunk < CHUNKS else lax.rem(q + chunk, SPAN // STEP)
                lanes = pl.ds(pl.multiple_of(lane * LANES, LANES), LANES)
            if chunk < CHUNKS:
                bands[t][b, rows, lanes] = pick(held, tables[phase, chunk])
            else:
                bands[t][b, rows, lanes] = jnp.zeros((EDGE, LANES), BF16)

    def wait_for(kind, b):
        for j in range(TILES):
            load(b, j, kind).wait()

    def mask_rows(b, total):
        for r in range(b * EDGE, (b + 1) * EDGE):
            row_gap = r - row_at[...]
            edge = bound - row_gap * row_gap
            for j in range(TILES):
                kept = jnp.where(col_sq[j] <= edge, prints[j, r].astype(F32), 0.0)
                foot[j, r] = kept.astype(BF16)
                total = total + kept * kept
        return total

    def first_residual(b):
        rows = slice(b * EDGE, (b + 1) * EDGE)
        feet = foot[:, rows].reshape(TILES * EDGE * EDGE, comps)
        prod = jnp.dot(feet, trace[...], preferred_element_type=F32)
        prod = prod.reshape(TILES, EDGE, EDGE, frames)
        for j in range(TILES):
            diff = prod[j] - movie[j, rows].astype(F32)
            pm[j, rows] = diff
            store_window(0, rows, j, diff)

    taps = stored.shape[0]
    run = CYCLE * SIDE
    for h in range(SIDE // CYCLE):
        values = stored[:, h * run : (h + 1) * run].astype(F32)
        values = jnp.concatenate([values, jnp.zeros((LANES - taps, run), F32)], axis=0)
        turned = jnp.transpose(values).astype(BF16)
        weights[h * CYCLE : (h + 1) * CYCLE] = turned.reshape(CYCLE, TILES, EDGE, LANES)
    wait_for(0, 0)
    total = mask_rows(0, jnp.zeros((EDGE, comps), F32))
    for b in range(TILES):
        wait_for(1, b)
        if b + 1 < TILES:
            wait_for(0, b + 1)
            total = mask_rows(b + 1, total)
        first_residual(b)
        for i in range(EDGE):
            weave(0, b, i // STEP, i % STEP)
    den = jnp.sum(total, axis=0, keepdims=True) + RIDGE_TERM
    inv_den[...] = jnp.transpose(jnp.broadcast_to(1.0 / den, (LANES, comps)))

    def halo_copy(sweep):
        return pltpu.make_async_remote_copy(
            src_ref=halo_out.at[sweep],
            dst_ref=halo_in.at[sweep],
            send_sem=halo_sems.at[0, sweep],
            recv_sem=halo_sems.at[1, sweep],
            device_id={"tile": 1 - tile},
            device_id_type=MESH,
        )

    def send_halo(sweep, diff):
        cut = jnp.where(tile == 0, diff[:, CYCLE:EDGE], diff[:, 0:CYCLE])
        halo_out[sweep] = (-cut).reshape(SIDE * CYCLE, frames).astype(BF16)
        halo_copy(sweep).start()

    for sweep in range(PASSES):
        if sweep == 0:
            pl.semaphore_wait(barrier, n)
            send_halo(0, pm[near[0]])
        else:
            for t in range(TILES):
                j = near[t]
                prod = jnp.dot(
                    foot[j].reshape(SIDE * EDGE, comps), trace[...], preferred_element_type=F32
                )
                diff = prod.reshape(SIDE, EDGE, frames) - movie[j].astype(F32)
                pm[j] = diff
                store_window(sweep, slice(0, SIDE), j, diff)
                if t == 0:
                    send_halo(sweep, diff)

        for t in range(TILES):
            j = near[TILES - 1 - t]
            if t == TILES - 1:
                halo_copy(sweep).wait_recv()
                came = halo_in[sweep].astype(F32).reshape(SIDE, CYCLE, frames).astype(BF16)

                @pl.when(tile == 0)
                def _():
                    win[sweep, :, TILES, CYCLE:EDGE] = came

                @pl.when(tile != 0)
                def _():
                    win[sweep, :, 0, 0:CYCLE] = came

            for b in range(TILES):
                if sweep == 0 and t + 1 < TILES:
                    for i in range(EDGE):
                        weave(t + 1, b, i // STEP, i % STEP)
                first = b * EDGE - CYCLE
                low, high = max(first, 0), min(first + SPAN, SIDE)
                seen = win[sweep, low:high, pl.ds(j, 2)].reshape((high - low) * SPAN, frames)
                taken = bands[t][b, :, (low - first) * SPAN : (high - first) * SPAN]
                back = jnp.dot(taken, seen, preferred_element_type=F32).astype(BF16)
                back = back.reshape(EDGE, EDGE, frames)
                rows = slice(b * EDGE, (b + 1) * EDGE)
                if sweep == PASSES - 1:
                    backs[j, rows] = back
                errs[j, rows] = (pm[j, rows] + back.astype(F32)).astype(BF16)

        grad = lax.dot_general(
            foot[...].reshape(pixels, comps),
            errs[...].reshape(pixels, frames),
            (((0,), (0,)), ((), ())),
            preferred_element_type=F32,
        )
        for q in range(frames // LANES):
            cols = slice(q * LANES, (q + 1) * LANES)
            moved = jnp.maximum(trace[:, cols].astype(F32) - grad[:, cols] * inv_den[...], 0.0)
            trace[:, cols] = jnp.where(live, moved, 0.0).astype(BF16)

    new_trace[...] = trace[...]
    squares = jnp.zeros((comps, LANES), F32)
    for q in range(frames // LANES):
        now = trace[:, q * LANES : (q + 1) * LANES].astype(F32)
        squares = squares + now * now
    energy = jnp.sum(jnp.transpose(squares), axis=0, keepdims=True)
    energy_out[...] = energy

    def energy_copy(peer, sender):
        return pltpu.make_async_remote_copy(
            src_ref=energy_out,
            dst_ref=energy_in.at[sender],
            send_sem=energy_sems.at[0, peer],
            recv_sem=energy_sems.at[1, sender],
            device_id={"tm": peer},
            device_id_type=MESH,
        )

    def lines(share):
        return slice(bounds[share] * EDGE, bounds[share + 1] * EDGE)

    def part_copy(share, sender):
        return pltpu.make_async_remote_copy(
            src_ref=part.at[lines(share)],
            dst_ref=arrived.at[sender, 0 : (bounds[share + 1] - bounds[share]) * EDGE],
            send_sem=part_sems.at[0, share],
            recv_sem=part_sems.at[1, sender],
            device_id={"tm": share},
            device_id_type=MESH,
        )

    def gather_copy(peer, share):
        return pltpu.make_async_remote_copy(
            src_ref=gathered.at[lines(share)],
            dst_ref=gathered.at[lines(share)],
            send_sem=gather_sems.at[0, peer],
            recv_sem=gather_sems.at[1, share],
            device_id={"tm": peer},
            device_id_type=MESH,
        )

    def over_peers(do):
        def step(t, carry):
            do(lax.rem(me + 1 + t, n))
            return carry

        lax.fori_loop(0, n - 1, step, 0)

    over_peers(lambda peer: energy_copy(peer, me).start())

    def rows_of(ref, runs):
        found = jnp.concatenate([ref[j, low:high] for j, low, high, _ in runs], axis=0)
        return found.reshape(found.shape[0] * EDGE, ref.shape[3])

    def fold(values, runs, first, last):
        values = values.reshape(-1, EDGE, comps)
        totals, at = [None] * (last - first), 0
        for _, low, high, row in runs:
            for index in range(row - first, row - first + high - low):
                totals[index] = values[at] if totals[index] is None else totals[index] + values[at]
                at += 1
        return totals

    def grads_of(first, last):
        runs = fold_runs(first, last)
        feet = rows_of(foot, runs)
        prod = jnp.dot(feet, trace[...], preferred_element_type=F32)
        ferr = prod + rows_of(backs, runs).astype(F32) - rows_of(movie, runs).astype(F32)
        grad = lax.dot_general(
            ferr.astype(BF16), trace[...], (((1,), (1,)), ((), ())), preferred_element_type=F32
        )
        return fold(jnp.where(feet.astype(F32) > 0.0, grad, 0.0), runs, first, last)

    owned = [share for share in range(n) if bounds[share] < bounds[share + 1]]
    teams = share_teams(bounds)
    for team in teams[::ORDER]:
        first, last = bounds[team[0]], bounds[team[-1] + 1]
        found = grads_of(first, last)
        for index in range(last - first):
            part[(first + index) * EDGE : (first + index + 1) * EDGE] = found[index].astype(BF16)
        for share in team:
            @pl.when(me != share)
            def _():
                part_copy(share, me).start()

            @pl.when(me == share)
            def _():
                for row in range(bounds[share], bounds[share + 1]):
                    at = (row - bounds[share]) * EDGE
                    own[at : at + EDGE] = found[row - first]

    energy_in[me] = energy_out[...]

    def take_energy(peer):
        energy_copy(me, peer).wait_recv()
        energy_in[me] += energy_in[peer]

    over_peers(take_energy)
    den_c = energy_in[me] + RIDGE_TERM

    def settle(share):
        first, last = bounds[share], bounds[share + 1]
        size = (last - first) * EDGE

        def take(peer):
            part_copy(share, peer).wait_recv()
            own[0:size] += arrived[peer, 0:size].astype(F32)

        over_peers(take)
        runs = fold_runs(first, last)
        feet = jnp.concatenate(fold(rows_of(foot, runs).astype(F32), runs, first, last), axis=0)
        gathered[lines(share)] = jnp.maximum(feet - own[0:size] / den_c, 0.0).astype(BF16)
        over_peers(lambda peer: gather_copy(peer, share).start())

    for share in owned:
        pl.when(me == share)(functools.partial(settle, share))
    for share in owned[::ORDER]:
        pl.when(me != share)(lambda: gather_copy(me, share).wait_recv())
        packed[lines(share)] = gathered[lines(share)]

    for sweep in range(PASSES):
        halo_copy(sweep).wait_send()

    over_peers(lambda peer: energy_copy(peer, me).wait_send())
    for share in owned:
        pl.when(me != share)(lambda: part_copy(share, me).wait_send())
        pl.when(me == share)(lambda: over_peers(lambda peer: gather_copy(peer, share).wait_send()))


def unfold(
    packed, trace, row_in, col_in, reach_in, count,
    new_foot, new_trace,
    row_at, col_at, reach, values, feet, load_sems, foot_sems,
):
    comps = feet.shape[2]
    loads = [
        pltpu.make_async_copy(source, target, load_sems.at[index])
        for index, (source, target) in enumerate((
            (trace, new_trace), (row_in, row_at), (col_in, col_at), (reach_in, reach),
        ))
    ]
    for copy in loads:
        copy.start()
    for copy in loads[1:]:
        copy.wait()
    live = lax.broadcasted_iota(jnp.int32, (1, comps), 1) < count[0]
    bound = jnp.where(live, reach[...] * reach[...], -1)
    for r in range(FOLD_ROWS):
        values[r] = packed[r * EDGE : (r + 1) * EDGE].astype(F32)
    col_sq = []
    for j in range(TILES):
        gap = lax.broadcasted_iota(jnp.int32, (EDGE, comps), 0) + j * EDGE - col_at[...]
        col_sq.append(gap * gap)

    def row(r):
        row_gap = r - row_at[...]
        edge = bound - row_gap * row_gap
        for j in range(TILES):
            value = values[lax.rem(r + (FOLD_ROWS - SHIFT) * j, FOLD_ROWS)]
            feet[r, j * EDGE : (j + 1) * EDGE] = jnp.where(col_sq[j] <= edge, value, 0.0).astype(BF16)

    copies = []
    for b in range(SIDE // CYCLE):
        def step(t, carry):
            for u in range(4):
                row(b * CYCLE + t * 4 + u)
            return carry

        lax.fori_loop(0, CYCLE // 4, step, 0)
        rows = slice(b * CYCLE, (b + 1) * CYCLE)
        copies.append(pltpu.make_async_copy(feet.at[rows], new_foot.at[rows], foot_sems.at[b]))
        copies[-1].start()
    for copy in copies:
        copy.wait()
    loads[0].wait()


def shards(movie, cycle_weights, footprints, traces, centre_row, centre_col, radius, comp_count):
    n = lax.axis_size("tm")
    frames = movie.shape[2]
    comps = footprints.shape[2]
    taps = cycle_weights.shape[2]
    bounds = share_bounds(n)
    widest = max(high - low for low, high in zip(bounds, bounds[1:])) * EDGE
    anyspace = pl.BlockSpec(memory_space=pl.ANY)
    smem = pl.BlockSpec(memory_space=pltpu.SMEM)
    dma = pltpu.SemaphoreType.DMA
    packed, trace = pl.pallas_call(
        functools.partial(kernel, n, bounds),
        out_shape=(
            pltpu.VMEM((FOLD_ROWS * EDGE, comps), BF16),
            pltpu.VMEM((comps, frames), BF16),
        ),
        in_specs=[anyspace] * 7 + [smem, anyspace],
        out_specs=(pl.BlockSpec(memory_space=pltpu.VMEM), pl.BlockSpec(memory_space=pltpu.VMEM)),
        scratch_shapes=[
            pltpu.VMEM((TILES, SIDE, EDGE, frames), BF16),
            pltpu.VMEM((taps, SIDE * SIDE), BF16),
            pltpu.VMEM((TILES, SIDE, EDGE, comps), BF16),
            pltpu.VMEM((comps, frames), BF16),
            pltpu.VMEM((1, comps), jnp.int32),
            pltpu.VMEM((1, comps), jnp.int32),
            pltpu.VMEM((1, comps), jnp.int32),
            pltpu.VMEM((STEP, CHUNKS, EDGE, LANES), jnp.int16),
            pltpu.VMEM((SIDE, TILES, EDGE, LANES), BF16),
            pltpu.VMEM((TILES, SIDE, EDGE, comps), BF16),
            pltpu.VMEM((TILES, EDGE * EDGE, SPAN * SPAN), BF16),
            pltpu.VMEM((TILES, EDGE * EDGE, SPAN * SPAN), BF16),
            pltpu.VMEM((TILES, EDGE * EDGE, SPAN * SPAN), BF16),
            pltpu.VMEM((TILES, SIDE, EDGE, frames), F32),
            pltpu.VMEM((PASSES, SIDE, TILES + 1, EDGE, frames), BF16),
            pltpu.VMEM((TILES, SIDE, EDGE, frames), BF16),
            pltpu.VMEM((TILES, SIDE, EDGE, frames), BF16),
            pltpu.VMEM((comps, LANES), F32),
            pltpu.VMEM((PASSES, SIDE * CYCLE, frames), BF16),
            pltpu.VMEM((PASSES, SIDE * CYCLE, frames), BF16),
            pltpu.VMEM((FOLD_ROWS * EDGE, comps), BF16),
            pltpu.VMEM((widest, comps), F32),
            pltpu.VMEM((n, widest, comps), BF16),
            pltpu.VMEM((1, comps), F32),
            pltpu.VMEM((n, 1, comps), F32),
            pltpu.VMEM((FOLD_ROWS * EDGE, comps), BF16),
            dma((2, TILES, TILES)),
            dma((6,)),
            dma((2, PASSES)),
            dma((2, n)),
            dma((2, n)),
            dma((2, n)),
        ],
        compiler_params=pltpu.CompilerParams(
            collective_id=0, has_side_effects=True, vmem_limit_bytes=62600000
        ),
    )(
        movie.reshape(SIDE, SIDE, frames),
        jnp.transpose(cycle_weights[0]),
        footprints.reshape(SIDE, SIDE, comps),
        traces.reshape(comps, frames),
        centre_row,
        centre_col,
        radius,
        comp_count,
        jnp.asarray(tap_tables()),
    )
    new_foot, new_trace = pl.pallas_call(
        unfold,
        out_shape=(
            jax.ShapeDtypeStruct((SIDE, SIDE, comps), BF16),
            jax.ShapeDtypeStruct((comps, frames), BF16),
        ),
        in_specs=[pl.BlockSpec(memory_space=pltpu.VMEM)] * 2 + [anyspace] * 3 + [smem],
        out_specs=(anyspace, anyspace),
        scratch_shapes=[
            pltpu.VMEM((1, comps), jnp.int32),
            pltpu.VMEM((1, comps), jnp.int32),
            pltpu.VMEM((1, comps), jnp.int32),
            pltpu.VMEM((FOLD_ROWS, EDGE, comps), F32),
            pltpu.VMEM((SIDE, SIDE, comps), BF16),
            dma((4,)),
            dma((SIDE // CYCLE,)),
        ],
        compiler_params=pltpu.CompilerParams(vmem_limit_bytes=12 * 1024 * 1024),
    )(packed, trace, centre_row, centre_col, radius, comp_count)
    return (new_foot.reshape(1, SIDE * SIDE, comps), new_trace[None])


def solution(mesh):
    in_specs = (
        P(("groups", "tile"), None, "tm"),
        P(("groups", "tile"), None, None),
        P(("groups", "tile"), None, None),
        P(("groups", "tile"), None, "tm"),
        P(("groups", "tile"), None),
        P(("groups", "tile"), None),
        P(("groups", "tile"), None),
        P(("groups", "tile")),
    )
    out_specs = (P(("groups", "tile"), None, None), P(("groups", "tile"), None, "tm"))
    return jax.shard_map(shards, mesh=mesh, in_specs=in_specs, out_specs=out_specs, check_vma=False)
```

```python
import functools

import jax
import jax.numpy as jnp
import numpy as np
from jax import lax
from jax.experimental import pallas as pl
from jax.experimental.pallas import tpu as pltpu
from jax.sharding import PartitionSpec as P

SIDE = 48
CYCLE = 8
PASSES = 2
RIDGE_TERM = 1.0
EDGE = 16
TILES = SIDE // EDGE
SPAN = EDGE + 2 * CYCLE
LANES = 128
STEP = LANES // SPAN
CHUNKS = (STEP - 1 + 2 * CYCLE) // STEP + 1
FOLD_ROWS = 19
SHIFT = 9
TEAM_ROWS = 4
ORDER = -1
F32 = jnp.float32
BF16 = jnp.bfloat16
MESH = pl.DeviceIdType.MESH


def cycle_offsets():
    found = []
    for row_step in range(-CYCLE, CYCLE + 1):
        for col_step in range(-CYCLE, CYCLE + 1):
            dist_sq = row_step * row_step + col_step * col_step
            if CYCLE * CYCLE <= dist_sq < (CYCLE + 1) * (CYCLE + 1):
                found.append((row_step, col_step))
    return found


def tap_tables():
    offsets = {step: index for index, step in enumerate(cycle_offsets())}
    tables = np.full((STEP, CHUNKS, EDGE, LANES), len(offsets), np.int16)
    for phase in range(STEP):
        for chunk in range(CHUNKS):
            for col in range(EDGE):
                for lane in range(LANES):
                    row_step = chunk * STEP + lane // SPAN - phase - CYCLE
                    col_step = lane % SPAN - col - CYCLE
                    if (row_step, col_step) in offsets:
                        tables[phase, chunk, col, lane] = offsets[(row_step, col_step)]
    return tables


def share_bounds(n):
    base, extra = divmod(FOLD_ROWS, n)
    bounds = [0]
    for index in range(n):
        bounds.append(bounds[-1] + base + (index >= n - extra))
    return bounds


def share_teams(bounds):
    teams, held = [], []
    for share in range(len(bounds) - 1):
        if bounds[share] < bounds[share + 1]:
            held.append(share)
        if held and bounds[share + 1] - bounds[held[0]] >= TEAM_ROWS:
            teams.append(held)
            held = []
    return teams + [held] if held else teams


def fold_runs(first, last):
    runs = []
    for j in range(TILES):
        for lap in range(-TILES, TILES + 1):
            moved = SHIFT * j + FOLD_ROWS * lap
            low, high = max(first + moved, 0), min(last + moved, SIDE)
            if low < high:
                runs.append((j, low, high, low - moved))
    return runs


def pick(values, index):
    numbers = lax.GatherDimensionNumbers(
        offset_dims=(), collapsed_slice_dims=(1,), start_index_map=(1,),
        operand_batching_dims=(0,), start_indices_batching_dims=(0,),
    )
    inside = lax.GatherScatterMode.PROMISE_IN_BOUNDS
    return lax.gather(values, index[..., None], numbers, (1, 1), mode=inside)


def kernel(
    n, bounds,
    movie_in, stored_in, prints_in, traces_in, row_in, col_in, reach_in, count, tables_in,
    packed, new_trace,
    movie, stored, prints, trace, row_at, col_at, reach, tables,
    weights, foot, band_first, band_second, band_third, pm, win, errs, backs, inv_den,
    halo_out, halo_in, part, own, arrived, energy_out, energy_in, gathered,
    load_sems, small_sems, halo_sems, part_sems, energy_sems, gather_sems,
):
    me = lax.axis_index("tm")
    tile = lax.axis_index("tile")
    frames = movie.shape[3]
    comps = foot.shape[3]
    pixels = SIDE * SIDE

    def load(b, j, kind):
        source, target = ((prints_in, prints), (movie_in, movie))[kind]
        rows = slice(b * EDGE, (b + 1) * EDGE)
        return pltpu.make_async_copy(
            source.at[rows, j * EDGE : (j + 1) * EDGE], target.at[j, rows], load_sems.at[kind, b, j]
        )

    smalls = [
        pltpu.make_async_copy(source, target, small_sems.at[index])
        for index, (source, target) in enumerate((
            (row_in, row_at), (col_in, col_at), (reach_in, reach),
            (stored_in, stored), (tables_in, tables), (traces_in, trace),
        ))
    ]
    for copy in smalls:
        copy.start()
    for b in range(TILES):
        for kind in range(2):
            for j in range(TILES):
                load(b, j, kind).start()

    barrier = pltpu.get_barrier_semaphore()
    pl.semaphore_signal(barrier, inc=1, device_id={"tile": 1 - tile}, device_id_type=MESH)

    def greet(t, carry):
        peer = lax.rem(me + 1 + t, n)
        pl.semaphore_signal(barrier, inc=1, device_id={"tm": peer}, device_id_type=MESH)
        return carry

    lax.fori_loop(0, n - 1, greet, 0)

    blank = jnp.zeros((SIDE, CYCLE, frames), BF16)
    for sweep in range(PASSES):
        win[sweep, :, 0, 0:CYCLE] = blank
        win[sweep, :, TILES, CYCLE:EDGE] = blank

    for copy in smalls:
        copy.wait()
    live_row = lax.broadcasted_iota(jnp.int32, (1, comps), 1) < count[0]
    bound = jnp.where(live_row, reach[...] * reach[...], -1)
    live = lax.broadcasted_iota(jnp.int32, (comps, LANES), 0) < count[0]
    for q in range(frames // LANES):
        cols = slice(q * LANES, (q + 1) * LANES)
        trace[:, cols] = jnp.where(live, trace[:, cols].astype(F32), 0.0).astype(BF16)

    col_sq = []
    for j in range(TILES):
        gap = lax.broadcasted_iota(jnp.int32, (EDGE, comps), 0) + j * EDGE - col_at[...]
        col_sq.append(gap * gap)

    def store_window(sweep, rows, j, diff):
        resid = (-diff).astype(BF16)
        win[sweep, rows, j, CYCLE:EDGE] = resid[:, 0:CYCLE]
        win[sweep, rows, j + 1, 0:CYCLE] = resid[:, CYCLE:EDGE]

    near = [jnp.where(tile == 0, TILES - 1 - t, t) for t in range(TILES)]
    bands = (band_first, band_second, band_third)

    def weave(t, b, q, phase):
        spot = (q * STEP + phase) * EDGE
        held = weights[b * EDGE + q * STEP + phase, near[TILES - 1 - t]]
        for chunk in range(SPAN // STEP):
            if isinstance(q, int):
                rows, lane = slice(spot, spot + EDGE), (q + chunk) % (SPAN // STEP) * LANES
                lanes = slice(lane, lane + LANES)
            else:
                rows = pl.ds(pl.multiple_of(spot, EDGE), EDGE)
                lane = q + chunk if chunk < CHUNKS else lax.rem(q + chunk, SPAN // STEP)
                lanes = pl.ds(pl.multiple_of(lane * LANES, LANES), LANES)
            if chunk < CHUNKS:
                bands[t][b, rows, lanes] = pick(held, tables[phase, chunk])
            else:
                bands[t][b, rows, lanes] = jnp.zeros((EDGE, LANES), BF16)

    def wait_for(kind, b):
        for j in range(TILES):
            load(b, j, kind).wait()

    def mask_rows(b, total):
        for r in range(b * EDGE, (b + 1) * EDGE):
            row_gap = r - row_at[...]
            edge = bound - row_gap * row_gap
            for j in range(TILES):
                kept = jnp.where(col_sq[j] <= edge, prints[j, r].astype(F32), 0.0)
                foot[j, r] = kept.astype(BF16)
                total = total + kept * kept
        return total

    def first_residual(b):
        rows = slice(b * EDGE, (b + 1) * EDGE)
        feet = foot[:, rows].reshape(TILES * EDGE * EDGE, comps)
        prod = jnp.dot(feet, trace[...], preferred_element_type=F32)
        prod = prod.reshape(TILES, EDGE, EDGE, frames)
        for j in range(TILES):
            diff = prod[j] - movie[j, rows].astype(F32)
            pm[j, rows] = diff
            store_window(0, rows, j, diff)

    taps = stored.shape[0]
    run = CYCLE * SIDE
    for h in range(SIDE // CYCLE):
        values = stored[:, h * run : (h + 1) * run].astype(F32)
        values = jnp.concatenate([values, jnp.zeros((LANES - taps, run), F32)], axis=0)
        turned = jnp.transpose(values).astype(BF16)
        weights[h * CYCLE : (h + 1) * CYCLE] = turned.reshape(CYCLE, TILES, EDGE, LANES)
    wait_for(0, 0)
    total = mask_rows(0, jnp.zeros((EDGE, comps), F32))
    for b in range(TILES):
        wait_for(1, b)
        if b + 1 < TILES:
            wait_for(0, b + 1)
            total = mask_rows(b + 1, total)
        first_residual(b)
        for i in range(EDGE):
            weave(0, b, i // STEP, i % STEP)
    den = jnp.sum(total, axis=0, keepdims=True) + RIDGE_TERM
    inv_den[...] = jnp.transpose(jnp.broadcast_to(1.0 / den, (LANES, comps)))

    def halo_copy(sweep):
        return pltpu.make_async_remote_copy(
            src_ref=halo_out.at[sweep],
            dst_ref=halo_in.at[sweep],
            send_sem=halo_sems.at[0, sweep],
            recv_sem=halo_sems.at[1, sweep],
            device_id={"tile": 1 - tile},
            device_id_type=MESH,
        )

    def send_halo(sweep, diff):
        cut = jnp.where(tile == 0, diff[:, CYCLE:EDGE], diff[:, 0:CYCLE])
        halo_out[sweep] = (-cut).reshape(SIDE * CYCLE, frames).astype(BF16)
        halo_copy(sweep).start()

    for sweep in range(PASSES):
        if sweep == 0:
            pl.semaphore_wait(barrier, n)
            send_halo(0, pm[near[0]])
        else:
            for t in range(TILES):
                j = near[t]
                prod = jnp.dot(
                    foot[j].reshape(SIDE * EDGE, comps), trace[...], preferred_element_type=F32
                )
                diff = prod.reshape(SIDE, EDGE, frames) - movie[j].astype(F32)
                pm[j] = diff
                store_window(sweep, slice(0, SIDE), j, diff)
                if t == 0:
                    send_halo(sweep, diff)

        for t in range(TILES):
            j = near[TILES - 1 - t]
            if t == TILES - 1:
                halo_copy(sweep).wait_recv()
                came = halo_in[sweep].astype(F32).reshape(SIDE, CYCLE, frames).astype(BF16)

                @pl.when(tile == 0)
                def _():
                    win[sweep, :, TILES, CYCLE:EDGE] = came

                @pl.when(tile != 0)
                def _():
                    win[sweep, :, 0, 0:CYCLE] = came

            for b in range(TILES):
                if sweep == 0 and t + 1 < TILES:
                    for i in range(EDGE):
                        weave(t + 1, b, i // STEP, i % STEP)
                first = b * EDGE - CYCLE
                low, high = max(first, 0), min(first + SPAN, SIDE)
                seen = win[sweep, low:high, pl.ds(j, 2)].reshape((high - low) * SPAN, frames)
                taken = bands[t][b, :, (low - first) * SPAN : (high - first) * SPAN]
                back = jnp.dot(taken, seen, preferred_element_type=F32).astype(BF16)
                back = back.reshape(EDGE, EDGE, frames)
                rows = slice(b * EDGE, (b + 1) * EDGE)
                if sweep == PASSES - 1:
                    backs[j, rows] = back
                errs[j, rows] = (pm[j, rows] + back.astype(F32)).astype(BF16)

        grad = lax.dot_general(
            foot[...].reshape(pixels, comps),
            errs[...].reshape(pixels, frames),
            (((0,), (0,)), ((), ())),
            preferred_element_type=F32,
        )
        for q in range(frames // LANES):
            cols = slice(q * LANES, (q + 1) * LANES)
            moved = jnp.maximum(trace[:, cols].astype(F32) - grad[:, cols] * inv_den[...], 0.0)
            trace[:, cols] = jnp.where(live, moved, 0.0).astype(BF16)

    new_trace[...] = trace[...]
    squares = jnp.zeros((comps, LANES), F32)
    for q in range(frames // LANES):
        now = trace[:, q * LANES : (q + 1) * LANES].astype(F32)
        squares = squares + now * now
    energy = jnp.sum(jnp.transpose(squares), axis=0, keepdims=True)
    energy_out[...] = energy

    def energy_copy(peer, sender):
        return pltpu.make_async_remote_copy(
            src_ref=energy_out,
            dst_ref=energy_in.at[sender],
            send_sem=energy_sems.at[0, peer],
            recv_sem=energy_sems.at[1, sender],
            device_id={"tm": peer},
            device_id_type=MESH,
        )

    def lines(share):
        return slice(bounds[share] * EDGE, bounds[share + 1] * EDGE)

    def part_copy(share, sender):
        return pltpu.make_async_remote_copy(
            src_ref=part.at[lines(share)],
            dst_ref=arrived.at[sender, 0 : (bounds[share + 1] - bounds[share]) * EDGE],
            send_sem=part_sems.at[0, share],
            recv_sem=part_sems.at[1, sender],
            device_id={"tm": share},
            device_id_type=MESH,
        )

    def gather_copy(peer, share):
        return pltpu.make_async_remote_copy(
            src_ref=gathered.at[lines(share)],
            dst_ref=gathered.at[lines(share)],
            send_sem=gather_sems.at[0, peer],
            recv_sem=gather_sems.at[1, share],
            device_id={"tm": peer},
            device_id_type=MESH,
        )

    def over_peers(do):
        def step(t, carry):
            do(lax.rem(me + 1 + t, n))
            return carry

        lax.fori_loop(0, n - 1, step, 0)

    over_peers(lambda peer: energy_copy(peer, me).start())

    def rows_of(ref, runs):
        found = jnp.concatenate([ref[j, low:high] for j, low, high, _ in runs], axis=0)
        return found.reshape(found.shape[0] * EDGE, ref.shape[3])

    def fold(values, runs, first, last):
        values = values.reshape(-1, EDGE, comps)
        totals, at = [None] * (last - first), 0
        for _, low, high, row in runs:
            for index in range(row - first, row - first + high - low):
                totals[index] = values[at] if totals[index] is None else totals[index] + values[at]
                at += 1
        return totals

    def grads_of(first, last):
        runs = fold_runs(first, last)
        feet = rows_of(foot, runs)
        prod = jnp.dot(feet, trace[...], preferred_element_type=F32)
        ferr = prod + rows_of(backs, runs).astype(F32) - rows_of(movie, runs).astype(F32)
        grad = lax.dot_general(
            ferr.astype(BF16), trace[...], (((1,), (1,)), ((), ())), preferred_element_type=F32
        )
        return fold(jnp.where(feet.astype(F32) > 0.0, grad, 0.0), runs, first, last)

    owned = [share for share in range(n) if bounds[share] < bounds[share + 1]]
    teams = share_teams(bounds)
    for team in teams[-2:] + teams[-3::-1]:
        first, last = bounds[team[0]], bounds[team[-1] + 1]
        found = grads_of(first, last)
        for index in range(last - first):
            part[(first + index) * EDGE : (first + index + 1) * EDGE] = found[index].astype(BF16)
        for share in team:
            @pl.when(me != share)
            def _():
                part_copy(share, me).start()

            @pl.when(me == share)
            def _():
                for row in range(bounds[share], bounds[share + 1]):
                    at = (row - bounds[share]) * EDGE
                    own[at : at + EDGE] = found[row - first]

    energy_in[me] = energy_out[...]

    def take_energy(peer):
        energy_copy(me, peer).wait_recv()
        energy_in[me] += energy_in[peer]

    over_peers(take_energy)
    den_c = energy_in[me] + RIDGE_TERM

    def settle(share):
        first, last = bounds[share], bounds[share + 1]
        size = (last - first) * EDGE

        def take(peer):
            part_copy(share, peer).wait_recv()
            own[0:size] += arrived[peer, 0:size].astype(F32)

        over_peers(take)
        runs = fold_runs(first, last)
        feet = jnp.concatenate(fold(rows_of(foot, runs).astype(F32), runs, first, last), axis=0)
        gathered[lines(share)] = jnp.maximum(feet - own[0:size] / den_c, 0.0).astype(BF16)
        over_peers(lambda peer: gather_copy(peer, share).start())

    for share in owned:
        pl.when(me == share)(functools.partial(settle, share))
    for share in owned[::ORDER]:
        pl.when(me != share)(lambda: gather_copy(me, share).wait_recv())
        packed[lines(share)] = gathered[lines(share)]

    for sweep in range(PASSES):
        halo_copy(sweep).wait_send()

    over_peers(lambda peer: energy_copy(peer, me).wait_send())
    for share in owned:
        pl.when(me != share)(lambda: part_copy(share, me).wait_send())
        pl.when(me == share)(lambda: over_peers(lambda peer: gather_copy(peer, share).wait_send()))


def unfold(
    packed, trace, row_in, col_in, reach_in, count,
    new_foot, new_trace,
    row_at, col_at, reach, values, feet, load_sems, foot_sems,
):
    comps = feet.shape[2]
    loads = [
        pltpu.make_async_copy(source, target, load_sems.at[index])
        for index, (source, target) in enumerate((
            (trace, new_trace), (row_in, row_at), (col_in, col_at), (reach_in, reach),
        ))
    ]
    for copy in loads:
        copy.start()
    for copy in loads[1:]:
        copy.wait()
    live = lax.broadcasted_iota(jnp.int32, (1, comps), 1) < count[0]
    bound = jnp.where(live, reach[...] * reach[...], -1)
    for r in range(FOLD_ROWS):
        values[r] = packed[r * EDGE : (r + 1) * EDGE].astype(F32)
    col_sq = []
    for j in range(TILES):
        gap = lax.broadcasted_iota(jnp.int32, (EDGE, comps), 0) + j * EDGE - col_at[...]
        col_sq.append(gap * gap)

    def row(r):
        row_gap = r - row_at[...]
        edge = bound - row_gap * row_gap
        for j in range(TILES):
            value = values[lax.rem(r + (FOLD_ROWS - SHIFT) * j, FOLD_ROWS)]
            feet[r, j * EDGE : (j + 1) * EDGE] = jnp.where(col_sq[j] <= edge, value, 0.0).astype(BF16)

    copies = []
    for b in range(SIDE // CYCLE):
        def step(t, carry):
            for u in range(4):
                row(b * CYCLE + t * 4 + u)
            return carry

        lax.fori_loop(0, CYCLE // 4, step, 0)
        rows = slice(b * CYCLE, (b + 1) * CYCLE)
        copies.append(pltpu.make_async_copy(feet.at[rows], new_foot.at[rows], foot_sems.at[b]))
        copies[-1].start()
    for copy in copies:
        copy.wait()
    loads[0].wait()


def shards(movie, cycle_weights, footprints, traces, centre_row, centre_col, radius, comp_count):
    n = lax.axis_size("tm")
    frames = movie.shape[2]
    comps = footprints.shape[2]
    taps = cycle_weights.shape[2]
    bounds = share_bounds(n)
    widest = max(high - low for low, high in zip(bounds, bounds[1:])) * EDGE
    anyspace = pl.BlockSpec(memory_space=pl.ANY)
    smem = pl.BlockSpec(memory_space=pltpu.SMEM)
    dma = pltpu.SemaphoreType.DMA
    packed, trace = pl.pallas_call(
        functools.partial(kernel, n, bounds),
        out_shape=(
            pltpu.VMEM((FOLD_ROWS * EDGE, comps), BF16),
            pltpu.VMEM((comps, frames), BF16),
        ),
        in_specs=[anyspace] * 7 + [smem, anyspace],
        out_specs=(pl.BlockSpec(memory_space=pltpu.VMEM), pl.BlockSpec(memory_space=pltpu.VMEM)),
        scratch_shapes=[
            pltpu.VMEM((TILES, SIDE, EDGE, frames), BF16),
            pltpu.VMEM((taps, SIDE * SIDE), BF16),
            pltpu.VMEM((TILES, SIDE, EDGE, comps), BF16),
            pltpu.VMEM((comps, frames), BF16),
            pltpu.VMEM((1, comps), jnp.int32),
            pltpu.VMEM((1, comps), jnp.int32),
            pltpu.VMEM((1, comps), jnp.int32),
            pltpu.VMEM((STEP, CHUNKS, EDGE, LANES), jnp.int16),
            pltpu.VMEM((SIDE, TILES, EDGE, LANES), BF16),
            pltpu.VMEM((TILES, SIDE, EDGE, comps), BF16),
            pltpu.VMEM((TILES, EDGE * EDGE, SPAN * SPAN), BF16),
            pltpu.VMEM((TILES, EDGE * EDGE, SPAN * SPAN), BF16),
            pltpu.VMEM((TILES, EDGE * EDGE, SPAN * SPAN), BF16),
            pltpu.VMEM((TILES, SIDE, EDGE, frames), F32),
            pltpu.VMEM((PASSES, SIDE, TILES + 1, EDGE, frames), BF16),
            pltpu.VMEM((TILES, SIDE, EDGE, frames), BF16),
            pltpu.VMEM((TILES, SIDE, EDGE, frames), BF16),
            pltpu.VMEM((comps, LANES), F32),
            pltpu.VMEM((PASSES, SIDE * CYCLE, frames), BF16),
            pltpu.VMEM((PASSES, SIDE * CYCLE, frames), BF16),
            pltpu.VMEM((FOLD_ROWS * EDGE, comps), BF16),
            pltpu.VMEM((widest, comps), F32),
            pltpu.VMEM((n, widest, comps), BF16),
            pltpu.VMEM((1, comps), F32),
            pltpu.VMEM((n, 1, comps), F32),
            pltpu.VMEM((FOLD_ROWS * EDGE, comps), BF16),
            dma((2, TILES, TILES)),
            dma((6,)),
            dma((2, PASSES)),
            dma((2, n)),
            dma((2, n)),
            dma((2, n)),
        ],
        compiler_params=pltpu.CompilerParams(
            collective_id=0, has_side_effects=True, vmem_limit_bytes=62600000
        ),
    )(
        movie.reshape(SIDE, SIDE, frames),
        jnp.transpose(cycle_weights[0]),
        footprints.reshape(SIDE, SIDE, comps),
        traces.reshape(comps, frames),
        centre_row,
        centre_col,
        radius,
        comp_count,
        jnp.asarray(tap_tables()),
    )
    new_foot, new_trace = pl.pallas_call(
        unfold,
        out_shape=(
            jax.ShapeDtypeStruct((SIDE, SIDE, comps), BF16),
            jax.ShapeDtypeStruct((comps, frames), BF16),
        ),
        in_specs=[pl.BlockSpec(memory_space=pltpu.VMEM)] * 2 + [anyspace] * 3 + [smem],
        out_specs=(anyspace, anyspace),
        scratch_shapes=[
            pltpu.VMEM((1, comps), jnp.int32),
            pltpu.VMEM((1, comps), jnp.int32),
            pltpu.VMEM((1, comps), jnp.int32),
            pltpu.VMEM((FOLD_ROWS, EDGE, comps), F32),
            pltpu.VMEM((SIDE, SIDE, comps), BF16),
            dma((4,)),
            dma((SIDE // CYCLE,)),
        ],
        compiler_params=pltpu.CompilerParams(vmem_limit_bytes=12 * 1024 * 1024),
    )(packed, trace, centre_row, centre_col, radius, comp_count)
    return (new_foot.reshape(1, SIDE * SIDE, comps), new_trace[None])


def solution(mesh):
    in_specs = (
        P(("groups", "tile"), None, "tm"),
        P(("groups", "tile"), None, None),
        P(("groups", "tile"), None, None),
        P(("groups", "tile"), None, "tm"),
        P(("groups", "tile"), None),
        P(("groups", "tile"), None),
        P(("groups", "tile"), None),
        P(("groups", "tile")),
    )
    out_specs = (P(("groups", "tile"), None, None), P(("groups", "tile"), None, "tm"))
    return jax.shard_map(shards, mesh=mesh, in_specs=in_specs, out_specs=out_specs, check_vma=False)
```
